32 devices in a mesh: gx: 4 (over x, core), gy: 4 (over z), gz: 2 (over y).
Axes of the slice: x: 2, y: 2, z: 4, core: 2. Of those that a mesh axis runs over, the one named last changes fastest.
Arguments:
- relative_placements: float32 [3, 12, 12, 8, 128], P(None, 'gx', 'gy', 'gz'), may hold values from 0 to 1
- mass_per_density: float32 [12, 12, 8, 128], P('gx', 'gy', 'gz'), may hold values from 0.004 to 0.04
- opening_heat_level: float32 [12, 12, 8, 128], P('gx', 'gy', 'gz'), may hold values from 0.5 to 2
- bin_fill_counts: int32 [12, 12, 8], P('gx', 'gy', 'gz'), may hold values from 16 to 128
Outputs:
- final_temp: float32 [12, 12, 8, 128], P('gx', 'gy', 'gz')
The draws below stay inside these ranges and needn't reach their ends.
Inputs may be any that keep to these rules, and one draw needn't show every extreme that they name: Tile cell t holds particles in slots 0 to bin_fill_counts[t] - 1; the other slots are empty and are no source.
All inputs are finite; a program needn't handle non-finite values.
Results may differ from the reference program's by a relative error of at most 0.0003.
Values sent between devices are 32-bit elements; how exact they have to be, the bound alone decides.
No kernel may reach another device: no remote copies, remote signals or barrier semaphores. Data moves between devices by JAX's collectives and lax.ppermute only.
A program may use at most 64 MiB of HBM per device.

```python
import math
import jax
import jax.numpy as jnp
from jax import lax

BIN_CAPACITY = 128
BLOCK_SPAN_EAST = 12
BLOCK_SPAN_NORTH = 12
BLOCK_SPAN_UPWARD = 8


def with_ends(drawn, own_key, least, largest):
    shape = drawn.shape
    spot = [jax.random.randint(jax.random.fold_in(own_key, axis), (), 0, shape[axis]) for axis in range(len(shape))]
    drawn = drawn.at[tuple(spot)].set(least)
    longest = shape.index(max(shape))
    spot[longest] = (spot[longest] + 1) % shape[longest]
    return drawn.at[tuple(spot)].set(largest)


def levels(rng, extent, split, least, largest):
    factor_of = 1.0
    for dim, shards_of in split:
        draws = jax.random.uniform(jax.random.fold_in(jax.random.fold_in(rng, 6), dim), (shards_of,), jnp.float32, least / len(split), largest / len(split))
        factor_of = factor_of * jnp.repeat(jnp.exp(draws), extent[dim] // shards_of).reshape((-1,) + (1,) * (len(extent) - 1 - dim))
    return factor_of


def setup_inputs(seed: int = 0) -> dict:
    keys = jax.random.split(jax.random.key(seed), 5)
    return {
        "relative_placements": jnp.clip(1.0 * jax.random.uniform(keys[0], (3, BLOCK_SPAN_EAST, BLOCK_SPAN_NORTH, BLOCK_SPAN_UPWARD, BIN_CAPACITY), jnp.float32) ** levels(keys[0], (3, BLOCK_SPAN_EAST, BLOCK_SPAN_NORTH, BLOCK_SPAN_UPWARD, BIN_CAPACITY), ((1, 4), (2, 4), (3, 2)), -0.2, 0.2), 0.0, 1.0),
        "mass_per_density": jnp.clip(jnp.exp(math.log(0.04) - 2.30258502 * jax.random.uniform(keys[1], (BLOCK_SPAN_EAST, BLOCK_SPAN_NORTH, BLOCK_SPAN_UPWARD, BIN_CAPACITY), jnp.float32) ** levels(keys[1], (BLOCK_SPAN_EAST, BLOCK_SPAN_NORTH, BLOCK_SPAN_UPWARD, BIN_CAPACITY), ((0, 4), (1, 4), (2, 2)), -0.2, 0.2)), 0.004, 0.04),
        "opening_heat_level": jnp.clip(jnp.exp(math.log(2.0) - 1.3862944 * jax.random.uniform(keys[2], (BLOCK_SPAN_EAST, BLOCK_SPAN_NORTH, BLOCK_SPAN_UPWARD, BIN_CAPACITY), jnp.float32) ** levels(keys[2], (BLOCK_SPAN_EAST, BLOCK_SPAN_NORTH, BLOCK_SPAN_UPWARD, BIN_CAPACITY), ((0, 4), (1, 4), (2, 2)), -0.2, 0.2)), 0.5, 2.0),
        "bin_fill_counts": with_ends(jax.random.randint(keys[3], (BLOCK_SPAN_EAST, BLOCK_SPAN_NORTH, BLOCK_SPAN_UPWARD), BIN_CAPACITY // 8, BIN_CAPACITY + 1), jax.random.fold_in(keys[3], 1), BIN_CAPACITY // 8, BIN_CAPACITY).astype(jnp.int32),
    }


step_factor = 2.0

def conduct(fields, periodic_enclosure):
    extent_x, extent_y, extent_z = periodic_enclosure
    bin_dimensions = fields.shape[-1]

    def one_column(column):
        col_x = column // extent_y
        col_y = column % extent_y

        def column_at(shift_x, shift_y):
            column_part = lax.dynamic_slice_in_dim(fields, col_x + 1 + shift_x, 1, 1)
            column_part = lax.dynamic_slice_in_dim(column_part, col_y + 1 + shift_y, 1, 2)
            return column_part[:, 0, 0]
        target = column_at(0, 0)[:, 1:1 + extent_z]
        inflow = jnp.zeros((extent_z, bin_dimensions), jnp.float32)
        weights = jnp.zeros((extent_z, bin_dimensions), jnp.float32)
        for shift_x in (-1, 0, 1):
            for shift_y in (-1, 0, 1):
                source_col = column_at(shift_x, shift_y)
                for shift_z in (-1, 0, 1):
                    source = source_col[:, 1 + shift_z:1 + shift_z + extent_z]
                    dist_sq = (float(shift_x) + source[0][:, None, :] - target[0][:, :, None]) ** 2
                    dist_sq = dist_sq + (float(shift_y) + source[1][:, None, :] - target[1][:, :, None]) ** 2
                    dist_sq = dist_sq + (float(shift_z) + source[2][:, None, :] - target[2][:, :, None]) ** 2
                    kernel = jnp.maximum(1.0 - jnp.sqrt(dist_sq), 0.0) ** 3
                    pair = kernel * source[3][:, None, :] * (target[5][:, :, None] + source[5][:, None, :])
                    inflow = inflow + lax.optimization_barrier(jnp.sum(pair * (source[4][:, None, :] - target[4][:, :, None]), axis=2))
                    weights = weights + lax.optimization_barrier(jnp.sum(pair, axis=2))
        return (inflow, weights)
    inflow, weights = lax.map(one_column, jnp.arange(extent_x * extent_y, dtype=jnp.int32))
    array_shape = (extent_x, extent_y, extent_z, bin_dimensions)
    return (inflow.reshape(array_shape), weights.reshape(array_shape))

def wrap_fields(relative_placements, smoothed_particle_measure, temp, heat_diffusion_coefficient):
    fields = jnp.concatenate([relative_placements, smoothed_particle_measure[None], temp[None], heat_diffusion_coefficient[None]], axis=0)
    return jnp.pad(fields, ((0, 0), (1, 1), (1, 1), (1, 1), (0, 0)), mode='wrap')

def reference(relative_placements, mass_per_density, opening_heat_level, bin_fill_counts):
    bin_dimensions = opening_heat_level.shape[-1]
    occupied = (jnp.arange(bin_dimensions, dtype=jnp.int32)[None, None, None, :] < bin_fill_counts[..., None]).astype(jnp.float32)
    smoothed_particle_measure = mass_per_density * occupied
    heat_diffusion_coefficient = opening_heat_level ** 2.5
    periodic_enclosure = opening_heat_level.shape[:3]
    opening_index = opening_heat_level
    reference_heat_rate, row_sums = conduct(wrap_fields(relative_placements, smoothed_particle_measure, opening_index, heat_diffusion_coefficient), periodic_enclosure)
    super_interval_length = step_factor / jnp.max(row_sums * occupied)
    leading_subset = opening_index + 2.0 / 15.0 * super_interval_length * reference_heat_rate
    initial_flow, unused_one = conduct(wrap_fields(relative_placements, smoothed_particle_measure, leading_subset, heat_diffusion_coefficient), periodic_enclosure)
    second = 1.5 * leading_subset - 0.5 * opening_index + 0.6 * super_interval_length * initial_flow - 0.4 * super_interval_length * reference_heat_rate
    flow_second, unused_two = conduct(wrap_fields(relative_placements, smoothed_particle_measure, second, heat_diffusion_coefficient), periodic_enclosure)
    final_temp = 25.0 / 12.0 * second - 5.0 / 6.0 * leading_subset - 0.25 * opening_index + 5.0 / 6.0 * super_interval_length * flow_second - 5.0 / 9.0 * super_interval_length * reference_heat_rate
    return final_temp
```

```python
import jax
import jax.numpy as jnp
from jax import lax
from jax.experimental import pallas as pl
from jax.experimental.pallas import tpu as pltpu
from jax.sharding import PartitionSpec as P

step_factor = 2.0
AXES = ("gx", "gy", "gz")
ROUNDER = 192.0
SHIFTS = (-1, 0, 1)
PAIRS = [(sx, sy) for sx in SHIFTS for sy in SHIFTS]


def swap_faces(value, axis, dim):
    size, length = lax.axis_size(axis), value.shape[dim]
    last = lax.slice_in_dim(value, length - 1, length, axis=dim)
    leading = lax.slice_in_dim(value, 0, 1, axis=dim)
    up = [(i, (i + 1) % size) for i in range(size)]
    if size == 2:
        both = lax.ppermute(jnp.concatenate([last, leading], axis=dim), axis, up)
        return lax.slice_in_dim(both, 0, 1, axis=dim), lax.slice_in_dim(both, 1, 2, axis=dim)
    down = [(j, i) for i, j in up]
    return lax.ppermute(last, axis, up), lax.ppermute(leading, axis, down)


def with_halo(value, first_dim):
    for place, axis in enumerate(AXES):
        dim = first_dim + place
        before, after = swap_faces(value, axis, dim)
        value = jnp.concatenate([before, value, after], axis=dim)
    return value


def rounded(x):
    return x.astype(jnp.bfloat16).astype(jnp.float32)


def split3(x):
    a = rounded(x)
    b = rounded(x - a)
    return a, b, x - a - b


def by_row(rows, row):
    out = rows[-1]
    for r in range(len(rows) - 2, -1, -1):
        out = jnp.where(row == r, rows[r], out)
    return out


class Sizes:
    def __init__(self, nx, ny, nz, slots):
        self.nx, self.ny, self.nz, self.slots = nx, ny, nz, slots
        self.px, self.py, self.pz = nx + 2, ny + 2, nz + 2
        self.cells = nx * ny * nz
        self.padded = self.px * self.py * self.pz
        self.half = nz // 2
        self.pairs = nx * ny * self.half
        self.columns = self.px * self.py

    def only_first(self):
        return 4 * self.slots * (4 * rounded_up(self.padded) + rounded_up(self.cells))

    def place(self, p):
        zp = p % self.half
        column = p // self.half
        return column // self.ny, column % self.ny, zp, column * self.nz + 2 * zp


def route(axis, distance):
    size = lax.axis_size(axis)
    return [(i, (i + distance) % size) for i in range(size)]


def rounded_up(rows):
    return -(-rows // 8) * 8


class Faces:
    def __init__(self, s):
        self.s = s
        self.x_rows = s.ny * s.nz
        self.y_rows = s.px * s.nz
        self.z_rows = s.px * s.py
        self.joined = lax.axis_size("gz") == 2

    def message(self, rows):
        return jax.ShapeDtypeStruct((rounded_up(rows + 1), self.s.slots), jnp.float32)

    def x_messages(self):
        return (self.message(self.x_rows),) * 2

    def y_messages(self):
        return (self.message(self.y_rows),) * 2

    def z_messages(self):
        return (self.message(2 * self.z_rows),) if self.joined else (self.message(self.z_rows),) * 2

    def row(self, x, y, z):
        return (x * self.s.py + y) * self.s.pz + z

    def put_own(self, halo, own):
        s = self.s
        for x in range(s.nx):
            for y in range(s.ny):
                at, start = self.row(x + 1, y + 1, 1), (x * s.ny + y) * s.nz
                halo[at : at + s.nz, :] = own[start : start + s.nz, :]

    def put_x(self, halo, before, after):
        s = self.s
        for side, x in ((before, 0), (after, s.nx + 1)):
            for y in range(s.ny):
                at = self.row(x, y + 1, 1)
                halo[at : at + s.nz, :] = side[y * s.nz : (y + 1) * s.nz, :]

    def put_y(self, halo, before, after):
        s = self.s
        for side, y in ((before, 0), (after, s.ny + 1)):
            for x in range(s.px):
                at = self.row(x, y, 1)
                halo[at : at + s.nz, :] = side[x * s.nz : (x + 1) * s.nz, :]

    def put_z(self, halo, sides):
        s = self.s
        for k, z in ((0, 0), (1, s.nz + 1)):
            side, base = (sides[0], k * self.z_rows) if self.joined else (sides[k], 0)
            for column in range(self.z_rows):
                halo[column * s.pz + z : column * s.pz + z + 1, :] = side[base + column : base + column + 1, :]

    def pack_x(self, own, top, up, down):
        s = self.s
        n = self.x_rows
        up[0:n, :] = own[(s.nx - 1) * n : s.nx * n, :]
        down[0:n, :] = own[0:n, :]
        for m in (up, down):
            m[n : n + 1, :] = top

    def pack_y(self, halo, top, up, down):
        s = self.s
        for x in range(s.px):
            for m, y in ((up, s.ny), (down, 1)):
                at = self.row(x, y, 1)
                m[x * s.nz : (x + 1) * s.nz, :] = halo[at : at + s.nz, :]
        for m in (up, down):
            m[self.y_rows : self.y_rows + 1, :] = top

    def pack_z(self, halo, top, messages):
        s = self.s
        for k, z in ((0, s.nz), (1, 1)):
            m, base = (messages[0], k * self.z_rows) if self.joined else (messages[k], 0)
            for column in range(self.z_rows):
                at = column * s.pz + z
                m[base + column : base + column + 1, :] = halo[at : at + 1, :]
        for m in messages:
            n = 2 * self.z_rows if self.joined else self.z_rows
            m[n : n + 1, :] = top

    def largest(self, rows, refs):
        return jnp.maximum(refs[0][rows : rows + 1, :], refs[-1][rows : rows + 1, :])

    def y_packer(self):
        s = self.s

        def body(own, top, before, after, up, down, top_out, halo):
            self.put_own(halo, own)
            self.put_x(halo, before, after)
            most = jnp.maximum(top[...], self.largest(self.x_rows, (before, after)))
            top_out[...] = most
            self.pack_y(halo, most, up, down)

        return pl.pallas_call(
            body,
            out_shape=(*self.y_messages(), jax.ShapeDtypeStruct((1, s.slots), jnp.float32)),
            scratch_shapes=[pltpu.VMEM((s.padded, s.slots), jnp.float32)],
            compiler_params=SMALL,
            name="pack_y",
        )

    def z_packer(self):
        s = self.s
        count = len(self.z_messages())

        def body(own, top, x0, x1, y0, y1, *rest):
            messages, top_out, halo = rest[:count], rest[count], rest[-1]
            self.put_own(halo, own)
            self.put_x(halo, x0, x1)
            self.put_y(halo, y0, y1)
            most = jnp.maximum(top[...], self.largest(self.y_rows, (y0, y1)))
            top_out[...] = most
            self.pack_z(halo, most, messages)

        return pl.pallas_call(
            body,
            out_shape=(*self.z_messages(), jax.ShapeDtypeStruct((1, s.slots), jnp.float32)),
            scratch_shapes=[pltpu.VMEM((s.padded, s.slots), jnp.float32)],
            compiler_params=SMALL,
            name="pack_z",
        )

    def exchange(self, own, top, up, down):
        x0 = lax.ppermute(up, "gx", route("gx", 1))
        x1 = lax.ppermute(down, "gx", route("gx", -1))
        up, down, top = self.y_packer()(own, top, x0, x1)
        y0 = lax.ppermute(up, "gy", route("gy", 1))
        y1 = lax.ppermute(down, "gy", route("gy", -1))
        *messages, top = self.z_packer()(own, top, x0, x1, y0, y1)
        if self.joined:
            z = (lax.ppermute(messages[0], "gz", route("gz", 1)),)
        else:
            z = (lax.ppermute(messages[0], "gz", route("gz", 1)), lax.ppermute(messages[1], "gz", route("gz", -1)))
        return (own, top, x0, x1, y0, y1, *z)

    def lay_out(self, halo, own, x0, x1, y0, y1, z):
        self.put_own(halo, own)
        self.put_x(halo, x0, x1)
        self.put_y(halo, y0, y1)
        self.put_z(halo, z)

    def latest_top(self, top, z):
        n = 2 * self.z_rows if self.joined else self.z_rows
        return jnp.maximum(top[...], self.largest(n, z))


SMALL = pltpu.CompilerParams(vmem_limit_bytes=2 << 20)
ROOM = 8 << 20


def weights_of(s, volume, conduct, temp, gains):
    row = lax.broadcasted_iota(jnp.int32, (8, s.slots), 0)
    use_c = (row % 4) < 2
    use_u = row < 4
    odd = (row % 2) == 1

    def one(cell, carry):
        def rows(ref):
            return jnp.broadcast_to(ref[pl.ds(cell, 1), :], (8, s.slots))

        full = rows(volume) * jnp.where(use_c, rows(conduct), 1.0)
        full = full * jnp.where(use_u, rows(temp), 1.0)
        top = rounded(full)
        gains[cell] = jnp.where(odd, full - top, top)
        return carry

    lax.fori_loop(0, s.padded, one, 0, unroll=6)


def gain_pair(gains, cell):
    both = jnp.concatenate([gains[cell], gains[cell + 1]], axis=0)
    return both.astype(jnp.bfloat16)


def keep_sums(s, total, own, sums):
    sums[own] = total[0:8, 0 : s.slots]
    sums[own + 1] = total[8:16, s.slots : 2 * s.slots]


def flow_from(s, sums_row, conduct_own, temp_own):
    def of(r):
        return sums_row(r)

    weight = of(4) + of(5) + conduct_own * (of(6) + of(7))
    flow = of(0) + of(1) + conduct_own * (of(2) + of(3)) - temp_own * weight
    return flow, weight


def first_kernel(s):
    slots = s.slots
    faces = Faces(s)

    def body(position, volume, temp, own_volume, own_temp, kernel_out, flow_out, conduct_out, top_out,
             up, down, left, gains, sums):
        conduct_out[...] = temp[...] * temp[...] * jnp.sqrt(temp[...])
        weights_of(s, volume, conduct_out, temp, gains)
        row = lax.broadcasted_iota(jnp.int32, (8, slots), 0)

        def axis_rows(cell, d):
            raw = position[d, pl.ds(cell, 1), :] - 0.5
            return jnp.broadcast_to((raw + ROUNDER) - ROUNDER, (8, slots))

        def features(column, carry):
            blocks = []
            for z in range(s.pz):
                cell = column * s.pz + z
                q = [axis_rows(cell, d) for d in range(3)]
                square = split3(q[0] * q[0] + q[1] * q[1] + q[2] * q[2])
                for d in range(3):
                    h = rounded(q[d])
                    m = q[d] - h
                    block = jnp.where(row % 2 == 0, h, m)
                    block = jnp.where(row < 4, block, jnp.where(row < 7, 1.0, square[d]))
                    blocks.append(block)
                blocks.append(jnp.zeros((8, slots), jnp.float32))
            for zp in range(s.half):
                quad = jnp.concatenate(blocks[8 * zp : 8 * zp + 16], axis=0)
                left[column * s.half + zp] = quad.T.astype(jnp.bfloat16)
            return carry

        lax.fori_loop(0, s.columns, features, 0)

        def target_rows(cell, d):
            q = axis_rows(cell, d)
            out = []
            for shift in SHIFTS:
                t = q - float(shift)
                h = rounded(t)
                m = t - h
                sq = split3(t * t)
                block = jnp.where(row < 2, -2.0 * h, -2.0 * m)
                rest = jnp.where(row == 4, sq[0], jnp.where(row == 5, sq[1], sq[2]))
                out.append(jnp.where(row < 4, block, jnp.where(row < 7, rest, 1.0)))
            return out

        nothing = jnp.zeros((16, slots), jnp.bfloat16)
        zero8 = jnp.zeros((8, slots), jnp.float32)

        def pair(p, carry):
            x, y, zp, own = s.place(p)
            centre = ((x + 1) * s.py + y + 1) * s.pz + 2 * zp + 1
            rows = [[target_rows(centre + k, d) for d in range(3)] for k in range(2)]
            low = [
                [[jnp.concatenate([rows[k][0][i], rows[k][1][j]], 0).astype(jnp.bfloat16) for j in range(3)]
                 for i in range(3)]
                for k in range(2)
            ]
            high = [
                [jnp.concatenate([rows[k][2][i], zero8], 0).astype(jnp.bfloat16) for i in range(3)]
                for k in range(2)
            ]
            total = jnp.zeros((16, 2 * slots), jnp.float32)
            for i in range(3):
                for j in range(3):
                    column = (x + i) * s.py + y + j
                    source = left[column * s.half + zp]
                    for e in range(3):
                        lanes = []
                        for k in range(2):
                            parts = [nothing] * 8
                            parts[2 * (e + k)] = low[k][i][j]
                            parts[2 * (e + k) + 1] = high[k][e]
                            lanes.append(jnp.concatenate(parts, axis=0))
                        right = jnp.concatenate(lanes, axis=1)
                        dist = jnp.dot(source, right, preferred_element_type=jnp.float32)
                        dist = jnp.maximum(dist, 1e-20)
                        gap = jnp.maximum(1.0 - dist * lax.rsqrt(dist), 0.0)
                        kernel = (gap * gap * gap).astype(jnp.bfloat16)
                        place = (i * 3 + j) * 3 + e
                        kernel_out[p, place * slots : (place + 1) * slots, :] = kernel
                        gain = gain_pair(gains, column * s.pz + 2 * zp + e)
                        total = total + jnp.dot(gain, kernel, preferred_element_type=jnp.float32)
            keep_sums(s, total, own, sums)
            return carry

        lax.fori_loop(0, s.pairs, pair, 0)

        def finish(cell, top):
            one = sums[cell]
            centre = own_cell(s, cell)
            flow, weight = flow_from(
                s, lambda r: one[r : r + 1, :], conduct_out[pl.ds(centre, 1), :], own_temp[pl.ds(cell, 1), :]
            )
            flow_out[pl.ds(cell, 1), :] = flow
            return jnp.maximum(top, jnp.where(own_volume[pl.ds(cell, 1), :] > 0.0, weight, 0.0))

        top = lax.fori_loop(0, s.cells, finish, jnp.zeros((1, slots), jnp.float32))
        top_out[...] = top
        faces.pack_x(flow_out, top, up, down)

    return pl.pallas_call(
        body,
        out_shape=(
            jax.ShapeDtypeStruct((s.pairs, 27 * slots, 2 * slots), jnp.bfloat16),
            jax.ShapeDtypeStruct((s.cells, slots), jnp.float32),
            jax.ShapeDtypeStruct((s.padded, slots), jnp.float32),
            jax.ShapeDtypeStruct((1, slots), jnp.float32),
            *faces.x_messages(),
        ),
        scratch_shapes=[
            pltpu.VMEM((s.columns * s.half, slots, 128), jnp.bfloat16),
            pltpu.VMEM((s.padded, 8, slots), jnp.float32),
            pltpu.VMEM((s.cells, 8, slots), jnp.float32),
        ],
        compiler_params=pltpu.CompilerParams(vmem_limit_bytes=ROOM),
        name="kernel_and_first_flow",
    )


def own_cell(s, cell):
    z = cell % s.nz
    column = cell // s.nz
    return ((column // s.ny + 1) * s.py + column % s.ny + 1) * s.pz + z + 1


def next_kernel(s, last):
    slots = s.slots
    faces = Faces(s)
    arrivals = len(faces.z_messages())

    def body(kernel, volume, conduct, own_temp, flow1, own, top, x0, x1, y0, y1, *rest):
        z, rest = rest[:arrivals], rest[arrivals:]
        if last:
            final_out, flow_out, temp, gains, sums = rest
        else:
            flow_out, top_out, up, down, temp, gains, sums = rest
        faces.lay_out(temp, own, x0, x1, y0, y1, z)
        most = faces.latest_top(top, z)
        weights_of(s, volume, conduct, temp, gains)

        def pair(p, carry):
            x, y, zp, cell = s.place(p)
            parts = []
            for i in range(3):
                for j in range(3):
                    for e in range(3):
                        source = ((x + i) * s.py + y + j) * s.pz + 2 * zp + e
                        parts.append(gain_pair(gains, source))
            gain = jnp.concatenate(parts, axis=1)
            total = jnp.dot(gain, kernel[p], preferred_element_type=jnp.float32)
            keep_sums(s, total, cell, sums)
            return carry

        lax.fori_loop(0, s.pairs, pair, 0)

        def finish(cell, carry):
            one = sums[cell]
            centre = own_cell(s, cell)
            flow, _ = flow_from(
                s, lambda r: one[r : r + 1, :], conduct[pl.ds(centre, 1), :], own[pl.ds(cell, 1), :]
            )
            flow_out[pl.ds(cell, 1), :] = flow
            return carry

        lax.fori_loop(0, s.cells, finish, 0)
        if last:
            if covered():
                step = step_factor / jnp.max(most, axis=1, keepdims=True)
                final_out[...] = polynomial(own_temp[...], step, flow1[...], own[...], flow_out[...])
        else:
            top_out[...] = most
            faces.pack_x(flow_out, most, up, down)

    flow_shape = jax.ShapeDtypeStruct((s.cells, slots), jnp.float32)
    if last:
        outs = (flow_shape, flow_shape)
    else:
        outs = (flow_shape, jax.ShapeDtypeStruct((1, slots), jnp.float32), *faces.x_messages())
    return pl.pallas_call(
        body,
        in_specs=[pl.BlockSpec(memory_space=pltpu.VMEM)] * (11 + arrivals),
        out_shape=outs,
        scratch_shapes=[
            pltpu.VMEM((s.padded, slots), jnp.float32),
            pltpu.VMEM((s.padded, 8, slots), jnp.float32),
            pltpu.VMEM((s.cells, 8, slots), jnp.float32),
        ],
        compiler_params=pltpu.CompilerParams(vmem_limit_bytes=ROOM + s.only_first()),
        name="last_flow" if last else "next_flow",
    )


def covered():
    return all(lax.axis_size(axis) <= 5 for axis in AXES)


def polynomial(start, step, flow1, flow2, flow3):
    return start + step * (flow1 + step * (0.5 * flow2 + step * (1.0 / 15.0) * flow3))


def local(relative_placements, mass_per_density, opening_heat_level, bin_fill_counts):
    nx, ny, nz, slots = opening_heat_level.shape
    s = Sizes(nx, ny, nz, slots)
    faces = Faces(s)
    occupied = jnp.arange(slots, dtype=jnp.int32) < bin_fill_counts[..., None]
    volume = jnp.where(occupied, mass_per_density, 0.0)
    fields = jnp.concatenate([relative_placements, volume[None], opening_heat_level[None]], axis=0)
    near = with_halo(fields, 1).reshape(5, s.padded, slots)
    own_volume = volume.reshape(s.cells, slots)
    own_temp = opening_heat_level.reshape(s.cells, slots)
    kernel, flow1, conduct, top, up, down = first_kernel(s)(near[:3], near[3], near[4], own_volume, own_temp)
    arrived = faces.exchange(flow1, top, up, down)
    flow2, top, up, down = next_kernel(s, False)(kernel, near[3], conduct, own_temp, flow1, *arrived)
    arrived = faces.exchange(flow2, top, up, down)
    final, flow3 = next_kernel(s, True)(kernel, near[3], conduct, own_temp, flow1, *arrived)
    if not covered():
        top, flow3 = lax.optimization_barrier((top, flow3))
        step = step_factor / lax.pmax(jnp.max(top), AXES)
        final = polynomial(own_temp, step, flow1, flow2, flow3)
    return final.reshape(nx, ny, nz, slots)


def solution(mesh):
    in_specs = (
        P(None, "gx", "gy", "gz", None),
        P("gx", "gy", "gz", None),
        P("gx", "gy", "gz", None),
        P("gx", "gy", "gz"),
    )
    out_specs = P("gx", "gy", "gz", None)
    return jax.shard_map(local, mesh=mesh, in_specs=in_specs, out_specs=out_specs, check_vma=False)
```

```python
import jax
import jax.numpy as jnp
from jax import lax
from jax.experimental import pallas as pl
from jax.experimental.pallas import tpu as pltpu
from jax.sharding import PartitionSpec as P

step_factor = 2.0
AXES = ("gx", "gy", "gz")
ROUNDER = 192.0
SHIFTS = (-1, 0, 1)
FIELDS = 5
ROOM = 8 << 20
SMALL = pltpu.CompilerParams(vmem_limit_bytes=2 << 20)


def route(axis, distance):
    size = lax.axis_size(axis)
    return [(i, (i + distance) % size) for i in range(size)]


def rounded_up(rows):
    return -(-rows // 8) * 8


def f32(*shape):
    return jax.ShapeDtypeStruct(shape, jnp.float32)


class Sizes:
    def __init__(self, nx, ny, nz, slots):
        self.nx, self.ny, self.nz, self.slots = nx, ny, nz, slots
        self.px, self.py, self.pz = nx + 2, ny + 2, nz + 2
        self.cells = nx * ny * nz
        self.padded = self.px * self.py * self.pz
        self.half = nz // 2
        self.pairs = nx * ny * self.half
        self.columns = self.px * self.py

    def place(self, p):
        zp = p % self.half
        column = p // self.half
        return column // self.ny, column % self.ny, zp, column * self.nz + 2 * zp


class Faces:
    def __init__(self, s, fields):
        self.s, self.fields = s, fields
        self.x_rows = s.ny * s.nz
        self.y_rows = s.px * s.nz
        self.joined = lax.axis_size("gz") == 2
        self.z_rows = s.px * s.py
        self.z_faces = 2 if self.joined else 1
        self.halo_shape = pltpu.VMEM((fields * s.padded, s.slots), jnp.float32)

    def message(self, rows):
        return f32(rounded_up(self.fields * rows + 1), self.s.slots)

    def x_messages(self):
        return (self.message(self.x_rows),) * 2

    def y_messages(self):
        return (self.message(self.y_rows),) * 2

    def z_messages(self):
        return (self.message(self.z_faces * self.z_rows),) * (2 // self.z_faces)

    def row(self, f, x, y, z):
        return f * self.s.padded + (x * self.s.py + y) * self.s.pz + z

    def put_own(self, halo, own):
        s = self.s
        for f in range(self.fields):
            for x in range(s.nx):
                for y in range(s.ny):
                    at, start = self.row(f, x + 1, y + 1, 1), f * s.cells + (x * s.ny + y) * s.nz
                    halo[at : at + s.nz, :] = own[start : start + s.nz, :]

    def put_x(self, halo, before, after):
        s = self.s
        for f in range(self.fields):
            for side, x in ((before, 0), (after, s.nx + 1)):
                for y in range(s.ny):
                    at, start = self.row(f, x, y + 1, 1), f * self.x_rows + y * s.nz
                    halo[at : at + s.nz, :] = side[start : start + s.nz, :]

    def put_y(self, halo, before, after):
        s = self.s
        for f in range(self.fields):
            for side, y in ((before, 0), (after, s.ny + 1)):
                for x in range(s.px):
                    at, start = self.row(f, x, y, 1), f * self.y_rows + x * s.nz
                    halo[at : at + s.nz, :] = side[start : start + s.nz, :]

    def z_places(self, below, above):
        for f in range(self.fields):
            for k, z in ((0, below), (1, above)):
                m, base = (0, k * self.z_rows) if self.joined else (k, 0)
                for column in range(self.z_rows):
                    yield m, f * self.z_faces * self.z_rows + base + column, f, column, z

    def put_z(self, halo, sides):
        for m, start, f, column, z in self.z_places(0, self.s.nz + 1):
            at = f * self.s.padded + column * self.s.pz + z
            halo[at : at + 1, :] = sides[m][start : start + 1, :]

    def end(self, message, rows, top):
        n = self.fields * rows
        message[n : n + 1, :] = top

    def pack_x(self, own, top, up, down):
        s = self.s
        n = self.x_rows
        for f in range(self.fields):
            up[f * n : f * n + n, :] = own[f * s.cells + (s.nx - 1) * n : f * s.cells + s.nx * n, :]
            down[f * n : f * n + n, :] = own[f * s.cells : f * s.cells + n, :]
        for m in (up, down):
            self.end(m, n, top)

    def pack_y(self, halo, top, up, down):
        s = self.s
        for f in range(self.fields):
            for x in range(s.px):
                for m, y in ((up, s.ny), (down, 1)):
                    at, start = self.row(f, x, y, 1), f * self.y_rows + x * s.nz
                    m[start : start + s.nz, :] = halo[at : at + s.nz, :]
        for m in (up, down):
            self.end(m, self.y_rows, top)

    def pack_z(self, halo, top, messages):
        for m, start, f, column, z in self.z_places(self.s.nz, 1):
            at = f * self.s.padded + column * self.s.pz + z
            messages[m][start : start + 1, :] = halo[at : at + 1, :]
        for m in messages:
            self.end(m, self.z_faces * self.z_rows, top)

    def largest(self, top, rows, refs):
        n = self.fields * rows
        return jnp.maximum(top[...], jnp.maximum(refs[0][n : n + 1, :], refs[-1][n : n + 1, :]))

    def y_packer(self):
        def body(own, top, before, after, up, down, top_out, halo):
            self.put_own(halo, own)
            self.put_x(halo, before, after)
            most = self.largest(top, self.x_rows, (before, after))
            top_out[...] = most
            self.pack_y(halo, most, up, down)

        return pl.pallas_call(
            body,
            out_shape=(*self.y_messages(), f32(1, self.s.slots)),
            scratch_shapes=[self.halo_shape],
            compiler_params=SMALL,
            name="pack_y",
        )

    def z_packer(self):
        count = len(self.z_messages())

        def body(own, top, x0, x1, y0, y1, *rest):
            messages, top_out, halo = rest[:count], rest[count], rest[-1]
            self.put_own(halo, own)
            self.put_x(halo, x0, x1)
            self.put_y(halo, y0, y1)
            most = self.largest(top, self.y_rows, (y0, y1))
            top_out[...] = most
            self.pack_z(halo, most, messages)

        return pl.pallas_call(
            body,
            out_shape=(*self.z_messages(), f32(1, self.s.slots)),
            scratch_shapes=[self.halo_shape],
            compiler_params=SMALL,
            name="pack_z",
        )

    def exchange(self, own, top, up, down):
        x0 = lax.ppermute(up, "gx", route("gx", 1))
        x1 = lax.ppermute(down, "gx", route("gx", -1))
        up, down, top = self.y_packer()(own, top, x0, x1)
        y0 = lax.ppermute(up, "gy", route("gy", 1))
        y1 = lax.ppermute(down, "gy", route("gy", -1))
        *messages, top = self.z_packer()(own, top, x0, x1, y0, y1)
        z = [lax.ppermute(m, "gz", route("gz", d)) for m, d in zip(messages, (1, -1))]
        return (own, top, x0, x1, y0, y1, *z)

    def lay_out(self, halo, own, x0, x1, y0, y1, z):
        self.put_own(halo, own)
        self.put_x(halo, x0, x1)
        self.put_y(halo, y0, y1)
        self.put_z(halo, z)

    def latest_top(self, top, z):
        return self.largest(top, self.z_faces * self.z_rows, z)


def rounded(x):
    return x.astype(jnp.bfloat16).astype(jnp.float32)


def split3(x):
    a = rounded(x)
    b = rounded(x - a)
    return a, b, x - a - b


def start_kernel(s):
    faces = Faces(s, FIELDS)

    def body(counts_in, placements_in, mass_in, temp_in, own, top_out, up, down,
             counts, placements, mass, temp, arrived):
        copies = [
            pltpu.make_async_copy(a, b, arrived.at[k])
            for k, (a, b) in enumerate(
                ((counts_in, counts), (placements_in, placements), (mass_in, mass), (temp_in, temp))
            )
        ]
        for copy in copies:
            copy.start()
        for copy in copies:
            copy.wait()
        slot = lax.broadcasted_iota(jnp.int32, (1, s.slots), 1)
        for x in range(s.nx):
            for y in range(s.ny):
                start = (x * s.ny + y) * s.nz
                for d in range(3):
                    own[d * s.cells + start : d * s.cells + start + s.nz, :] = placements[d, x, y]
                rows = [
                    jnp.where(slot < counts[x, y, z], mass[x, y, z : z + 1, :], 0.0) for z in range(s.nz)
                ]
                own[3 * s.cells + start : 3 * s.cells + start + s.nz, :] = jnp.concatenate(rows, axis=0)
                own[4 * s.cells + start : 4 * s.cells + start + s.nz, :] = temp[x, y]
        none = jnp.zeros((1, s.slots), jnp.float32)
        top_out[...] = none
        faces.pack_x(own, none, up, down)

    block = (s.nx, s.ny, s.nz, s.slots)
    return pl.pallas_call(
        body,
        in_specs=[pl.BlockSpec(memory_space=pltpu.HBM)] * 4,
        out_shape=(f32(FIELDS * s.cells, s.slots), f32(1, s.slots), *faces.x_messages()),
        scratch_shapes=[
            pltpu.SMEM(block[:3], jnp.int32),
            pltpu.VMEM((3, *block), jnp.float32),
            pltpu.VMEM(block, jnp.float32),
            pltpu.VMEM(block, jnp.float32),
            pltpu.SemaphoreType.DMA((4,)),
        ],
        compiler_params=SMALL,
        name="start",
    )


def source_rows(s, volume, scaled, temp, gains):
    row = lax.broadcasted_iota(jnp.int32, (8, s.slots), 0)
    use_c = (row % 4) < 2
    use_u = row < 4
    odd = (row % 2) == 1

    def one(cell, carry):
        def rows(ref):
            return jnp.broadcast_to(ref[pl.ds(cell, 1), :], (8, s.slots))

        full = jnp.where(use_c, rows(scaled), rows(volume)) * jnp.where(use_u, rows(temp), 1.0)
        top = rounded(full)
        gains[cell] = jnp.where(odd, full - top, top)
        return carry

    lax.fori_loop(0, s.padded, one, 0, unroll=6)


def gain_pair(gains, cell):
    return jnp.concatenate([gains[cell], gains[cell + 1]], axis=0).astype(jnp.bfloat16)


def keep_sums(s, total, own, sums):
    sums[pl.ds(pl.multiple_of(own * 8, 8), 8), :] = total[0:8, 0 : s.slots]
    sums[pl.ds(pl.multiple_of(own * 8 + 8, 8), 8), :] = total[8:16, s.slots : 2 * s.slots]


def flow_of(s, sums, conduct_own, temp_own):
    def of(r):
        return sums[pl.ds(r, s.cells, stride=8), :]

    weight = of(4) + of(5) + conduct_own * (of(6) + of(7))
    flow = of(0) + of(1) + conduct_own * (of(2) + of(3)) - temp_own * weight
    return flow, weight


def gathered(s, gains, kernel, p, x, y, zp):
    parts = []
    for i in range(3):
        for j in range(3):
            for e in range(3):
                parts.append(gain_pair(gains, ((x + i) * s.py + y + j) * s.pz + 2 * zp + e))
    return jnp.dot(jnp.concatenate(parts, axis=1), kernel[p], preferred_element_type=jnp.float32)


def conductivity(temp):
    return temp * temp * jnp.sqrt(temp)


def first_kernel(s):
    slots = s.slots
    fields = Faces(s, FIELDS)
    faces = Faces(s, 1)
    arrivals = len(fields.z_messages())
    inputs = 4 * slots * sum(
        rounded_up(m.shape[0])
        for m in (f32(FIELDS * s.cells), *fields.x_messages(), *fields.y_messages(), *fields.z_messages())
    )

    def body(own, x0, x1, y0, y1, *rest):
        z, rest = rest[:arrivals], rest[arrivals:]
        (kernel_out, flow_out, volume_out, scaled_out, conduct_own, temp_own, top_out, up, down,
         halo, left, gains, sums, halves, targets) = rest
        fields.lay_out(halo, own, x0, x1, y0, y1, z)
        temp = halo.at[pl.ds(4 * s.padded, s.padded)]
        volume_out[...] = halo[3 * s.padded : 4 * s.padded, :]
        scaled_out[...] = volume_out[...] * conductivity(temp[...])
        temp_own[...] = own[4 * s.cells : 5 * s.cells, :]
        conduct_own[...] = conductivity(temp_own[...])
        source_rows(s, volume_out, scaled_out, temp, gains)
        row = lax.broadcasted_iota(jnp.int32, (8, slots), 0)

        even = row % 2 == 0
        square = 0.0
        for d in range(3):
            q = (halo[d * s.padded : (d + 1) * s.padded, :] - 0.5 + ROUNDER) - ROUNDER
            halves[2 * d] = rounded(q)
            halves[2 * d + 1] = q - rounded(q)
            square = square + q * q
            q = (own[d * s.cells : (d + 1) * s.cells, :] - 0.5 + ROUNDER) - ROUNDER
            for k, shift in enumerate(SHIFTS):
                t = q - float(shift)
                h = rounded(t)
                for r, part in enumerate((-2.0 * h, -2.0 * (t - h), *split3(t * t))):
                    targets[(d * 3 + k) * 5 + r] = part
        for d, part in enumerate(split3(square)):
            halves[6 + d] = part

        def spread(ref, k, cell):
            return jnp.broadcast_to(ref[k, pl.ds(cell, 1), :], (8, slots))

        def features(column, carry):
            blocks = []
            for z in range(s.pz):
                cell = column * s.pz + z
                for d in range(3):
                    block = jnp.where(even, spread(halves, 2 * d, cell), spread(halves, 2 * d + 1, cell))
                    rest = jnp.where(row < 7, 1.0, spread(halves, 6 + d, cell))
                    blocks.append(jnp.where(row < 4, block, rest))
                blocks.append(jnp.zeros((8, slots), jnp.float32))
            for zp in range(s.half):
                quad = jnp.concatenate(blocks[8 * zp : 8 * zp + 16], axis=0)
                left[column * s.half + zp] = quad.T.astype(jnp.bfloat16)
            return carry

        lax.fori_loop(0, s.columns, features, 0, unroll=5)

        def target_rows(cell, d):
            out = []
            for k in range(3):
                part = [spread(targets, (d * 3 + k) * 5 + r, cell) for r in range(5)]
                block = jnp.where(row == 5, part[3], jnp.where(row == 6, part[4], 1.0))
                block = jnp.where(row < 4, part[1], jnp.where(row == 4, part[2], block))
                out.append(jnp.where(row < 2, part[0], block))
            return out

        nothing = jnp.zeros((16, slots), jnp.bfloat16)
        zero8 = jnp.zeros((8, slots), jnp.float32)

        def pair(p, carry):
            x, y, zp, cell = s.place(p)
            rows = [[target_rows(cell + k, d) for d in range(3)] for k in range(2)]
            low = [
                [[jnp.concatenate([rows[k][0][i], rows[k][1][j]], 0).astype(jnp.bfloat16) for j in range(3)]
                 for i in range(3)]
                for k in range(2)
            ]
            high = [
                [jnp.concatenate([rows[k][2][i], zero8], 0).astype(jnp.bfloat16) for i in range(3)]
                for k in range(2)
            ]
            for i in range(3):
                for j in range(3):
                    source = left[((x + i) * s.py + y + j) * s.half + zp]
                    for e in range(3):
                        lanes = []
                        for k in range(2):
                            parts = [nothing] * 8
                            parts[2 * (e + k)] = low[k][i][j]
                            parts[2 * (e + k) + 1] = high[k][e]
                            lanes.append(jnp.concatenate(parts, axis=0))
                        right = jnp.concatenate(lanes, axis=1)
                        dist = jnp.dot(source, right, preferred_element_type=jnp.float32)
                        gap = 1.0 - dist * lax.rsqrt(jnp.maximum(dist, 2.5e-7))
                        kernel = jnp.maximum((gap * gap * gap).astype(jnp.bfloat16), jnp.bfloat16(0.0))
                        at = ((i * 3 + j) * 3 + e) * slots
                        kernel_out[p, at : at + slots, :] = kernel
            keep_sums(s, gathered(s, gains, kernel_out, p, x, y, zp), cell, sums)
            return carry

        lax.fori_loop(0, s.pairs, pair, 0, unroll=2)

        flow, weight = flow_of(s, sums, conduct_own[...], temp_own[...])
        flow_out[...] = flow
        occupied = own[3 * s.cells : 4 * s.cells, :] > 0.0
        top = jnp.max(jnp.where(occupied, weight, 0.0), axis=0, keepdims=True)
        top_out[...] = top
        faces.pack_x(flow_out, top, up, down)

    cells, padded = f32(s.cells, slots), f32(s.padded, slots)
    call = pl.pallas_call(
        body,
        out_shape=(
            jax.ShapeDtypeStruct((s.pairs, 27 * slots, 2 * slots), jnp.bfloat16),
            cells,
            padded,
            padded,
            cells,
            cells,
            f32(1, slots),
            *faces.x_messages(),
        ),
        scratch_shapes=[
            fields.halo_shape,
            pltpu.VMEM((s.columns * s.half, slots, 128), jnp.bfloat16),
            pltpu.VMEM((s.padded, 8, slots), jnp.float32),
            pltpu.VMEM((s.cells * 8, slots), jnp.float32),
            pltpu.VMEM((9, s.padded, slots), jnp.float32),
            pltpu.VMEM((45, s.cells, slots), jnp.float32),
        ],
        compiler_params=pltpu.CompilerParams(vmem_limit_bytes=ROOM),
        name="kernel_and_first_flow",
    )
    return call, inputs


def next_kernel(s, room, last):
    slots = s.slots
    faces = Faces(s, 1)
    arrivals = len(faces.z_messages())

    def body(kernel, volume, scaled, conduct_own, *rest):
        if last:
            temp_own, flow1, *rest = rest
        own, top, x0, x1, y0, y1, *rest = rest
        z, rest = rest[:arrivals], rest[arrivals:]
        if last:
            out, temp, gains, sums, *rest = rest
        else:
            flow_out, top_out, up, down, temp, gains, sums = rest
        faces.lay_out(temp, own, x0, x1, y0, y1, z)
        most = faces.latest_top(top, z)
        source_rows(s, volume, scaled, temp, gains)

        def pair(p, carry):
            x, y, zp, cell = s.place(p)
            keep_sums(s, gathered(s, gains, kernel, p, x, y, zp), cell, sums)
            return carry

        lax.fori_loop(0, s.pairs, pair, 0)
        flow, _ = flow_of(s, sums, conduct_own[...], own[...])
        if last and covered():
            rows, block, arrived = rest
            step = step_factor / jnp.max(most, axis=1, keepdims=True)
            rows[...] = polynomial(temp_own[...], step, flow1[...], own[...], flow)
            for x in range(s.nx):
                for y in range(s.ny):
                    start = (x * s.ny + y) * s.nz
                    block[x, y] = rows[start : start + s.nz, :]
            copy = pltpu.make_async_copy(block, out, arrived)
            copy.start()
            copy.wait()
        elif last:
            out[...] = flow
        else:
            flow_out[...] = flow
            top_out[...] = most
            faces.pack_x(flow_out, most, up, down)

    cells, shape = f32(s.cells, slots), (s.nx, s.ny, s.nz, slots)
    outs = (cells, f32(1, slots), *faces.x_messages())
    spaces = [pltpu.VMEM] * len(outs)
    scratch = [
        faces.halo_shape,
        pltpu.VMEM((s.padded, 8, slots), jnp.float32),
        pltpu.VMEM((s.cells * 8, slots), jnp.float32),
    ]
    if last and covered():
        outs, spaces = (f32(*shape),), [pl.ANY]
        scratch += [pltpu.VMEM((s.cells, slots), jnp.float32), pltpu.VMEM(shape, jnp.float32), pltpu.SemaphoreType.DMA]
    elif last:
        outs, spaces = (cells,), [pltpu.VMEM]
    return pl.pallas_call(
        body,
        out_shape=outs,
        out_specs=tuple(pl.BlockSpec(memory_space=space) for space in spaces),
        scratch_shapes=scratch,
        compiler_params=pltpu.CompilerParams(vmem_limit_bytes=room),
        name="last_flow" if last else "next_flow",
    )


def covered():
    return all(lax.axis_size(axis) <= 5 for axis in AXES)


def polynomial(start, step, flow1, flow2, flow3):
    return start + step * (flow1 + step * (0.5 * flow2 + step * (1.0 / 15.0) * flow3))


def local(relative_placements, mass_per_density, opening_heat_level, bin_fill_counts):
    nx, ny, nz, slots = opening_heat_level.shape
    s = Sizes(nx, ny, nz, slots)
    fields, faces = Faces(s, FIELDS), Faces(s, 1)
    arguments = (bin_fill_counts, relative_placements, mass_per_density, opening_heat_level)
    started = start_kernel(s)(*[pltpu.with_memory_space_constraint(a, pltpu.HBM) for a in arguments])
    own, _, *messages = fields.exchange(*started)
    first, inputs = first_kernel(s)
    kernel, flow1, volume, scaled, conduct_own, temp_own, top, up, down = first(own, *messages)
    arrived = faces.exchange(flow1, top, up, down)
    flow2, top, up, down = next_kernel(s, ROOM + inputs, False)(kernel, volume, scaled, conduct_own, *arrived)
    arrived = faces.exchange(flow2, top, up, down)
    (final,) = next_kernel(s, ROOM + inputs, True)(
        kernel, volume, scaled, conduct_own, temp_own, flow1, *arrived
    )
    if not covered():
        top, flow3 = lax.optimization_barrier((arrived[1], final))
        step = step_factor / lax.pmax(jnp.max(top), AXES)
        final = polynomial(temp_own, step, flow1, flow2, flow3).reshape(nx, ny, nz, slots)
    return final


def solution(mesh):
    in_specs = (
        P(None, "gx", "gy", "gz", None),
        P("gx", "gy", "gz", None),
        P("gx", "gy", "gz", None),
        P("gx", "gy", "gz"),
    )
    out_specs = P("gx", "gy", "gz", None)
    return jax.shard_map(local, mesh=mesh, in_specs=in_specs, out_specs=out_specs, check_vma=False)
```

```python
import functools

import jax
import jax.numpy as jnp
from jax import lax
from jax.experimental import pallas as pl
from jax.experimental.pallas import tpu as pltpu
from jax.sharding import PartitionSpec as P

step_factor = 2.0
AXES = ("gx", "gy", "gz")
ROUNDER = 192.0
SHIFTS = (-1, 0, 1)
FIELDS = 5
ROOM = 8 << 20
SMALL = pltpu.CompilerParams(vmem_limit_bytes=2 << 20)


def route(axis, distance):
    size = lax.axis_size(axis)
    return [(i, (i + distance) % size) for i in range(size)]


def rounded_up(rows):
    return -(-rows // 8) * 8


def f32(*shape):
    return jax.ShapeDtypeStruct(shape, jnp.float32)


class Sizes:
    def __init__(self, nx, ny, nz, slots):
        self.nx, self.ny, self.nz, self.slots = nx, ny, nz, slots
        self.px, self.py, self.pz = nx + 2, ny + 2, nz + 2
        self.cells = nx * ny * nz
        self.padded = self.px * self.py * self.pz
        self.half = nz // 2
        self.pairs = nx * ny * self.half
        self.columns = self.px * self.py


class Faces:
    def __init__(self, s, fields):
        self.s, self.fields = s, fields
        self.x_rows = s.ny * s.nz
        self.y_rows = s.px * s.nz
        self.joined = lax.axis_size("gz") == 2
        self.z_rows = s.px * s.py
        self.z_faces = 2 if self.joined else 1
        self.halo_shape = pltpu.VMEM((fields * s.padded, s.slots), jnp.float32)

    def message(self, rows):
        return f32(rounded_up(self.fields * rows + 1), self.s.slots)

    def x_messages(self):
        return (self.message(self.x_rows),) * 2

    def y_messages(self):
        return (self.message(self.y_rows),) * 2

    def z_messages(self):
        return (self.message(self.z_faces * self.z_rows),) * (2 // self.z_faces)

    def row(self, f, x, y, z):
        return f * self.s.padded + (x * self.s.py + y) * self.s.pz + z

    def put_own(self, halo, own):
        s = self.s
        for f in range(self.fields):
            for x in range(s.nx):
                for y in range(s.ny):
                    at, start = self.row(f, x + 1, y + 1, 1), f * s.cells + (x * s.ny + y) * s.nz
                    halo[at : at + s.nz, :] = own[start : start + s.nz, :]

    def put_x(self, halo, before, after):
        s = self.s
        for f in range(self.fields):
            for side, x in ((before, 0), (after, s.nx + 1)):
                for y in range(s.ny):
                    at, start = self.row(f, x, y + 1, 1), f * self.x_rows + y * s.nz
                    halo[at : at + s.nz, :] = side[start : start + s.nz, :]

    def put_y(self, halo, before, after):
        s = self.s
        for f in range(self.fields):
            for side, y in ((before, 0), (after, s.ny + 1)):
                for x in range(s.px):
                    at, start = self.row(f, x, y, 1), f * self.y_rows + x * s.nz
                    halo[at : at + s.nz, :] = side[start : start + s.nz, :]

    def z_places(self, below, above):
        for f in range(self.fields):
            for k, z in ((0, below), (1, above)):
                m, base = (0, k * self.z_rows) if self.joined else (k, 0)
                for column in range(self.z_rows):
                    yield m, f * self.z_faces * self.z_rows + base + column, f, column, z

    def put_z(self, halo, sides):
        for m, start, f, column, z in self.z_places(0, self.s.nz + 1):
            at = f * self.s.padded + column * self.s.pz + z
            halo[at : at + 1, :] = sides[m][start : start + 1, :]

    def end(self, message, rows, top):
        n = self.fields * rows
        message[n : n + 1, :] = top

    def pack_x(self, own, top, up, down):
        s = self.s
        n = self.x_rows
        for f in range(self.fields):
            up[f * n : f * n + n, :] = own[f * s.cells + (s.nx - 1) * n : f * s.cells + s.nx * n, :]
            down[f * n : f * n + n, :] = own[f * s.cells : f * s.cells + n, :]
        for m in (up, down):
            self.end(m, n, top)

    def pack_y(self, halo, top, up, down):
        s = self.s
        for f in range(self.fields):
            for x in range(s.px):
                for m, y in ((up, s.ny), (down, 1)):
                    at, start = self.row(f, x, y, 1), f * self.y_rows + x * s.nz
                    m[start : start + s.nz, :] = halo[at : at + s.nz, :]
        for m in (up, down):
            self.end(m, self.y_rows, top)

    def pack_z(self, halo, top, messages):
        for m, start, f, column, z in self.z_places(self.s.nz, 1):
            at = f * self.s.padded + column * self.s.pz + z
            messages[m][start : start + 1, :] = halo[at : at + 1, :]
        for m in messages:
            self.end(m, self.z_faces * self.z_rows, top)

    def largest(self, top, rows, refs):
        n = self.fields * rows
        return jnp.maximum(top[...], jnp.maximum(refs[0][n : n + 1, :], refs[-1][n : n + 1, :]))

    def y_packer(self, waits):
        def body(own, top, before, after, *rest):
            up, down, top_out, halo = rest[waits:]
            self.put_own(halo, own)
            self.put_x(halo, before, after)
            most = self.largest(top, self.x_rows, (before, after))
            top_out[...] = most
            self.pack_y(halo, most, up, down)

        return pl.pallas_call(
            body,
            out_shape=(*self.y_messages(), f32(1, self.s.slots)),
            scratch_shapes=[self.halo_shape],
            compiler_params=SMALL,
            name="pack_y",
        )

    def z_packer(self, waits):
        count = len(self.z_messages())

        def body(own, top, x0, x1, y0, y1, *rest):
            rest = rest[waits:]
            messages, top_out, halo = rest[:count], rest[count], rest[-1]
            self.put_own(halo, own)
            self.put_x(halo, x0, x1)
            self.put_y(halo, y0, y1)
            most = self.largest(top, self.y_rows, (y0, y1))
            top_out[...] = most
            self.pack_z(halo, most, messages)

        return pl.pallas_call(
            body,
            out_shape=(*self.z_messages(), f32(1, self.s.slots)),
            scratch_shapes=[self.halo_shape],
            compiler_params=SMALL,
            name="pack_z",
        )

    def exchange(self, own, top, up, down, during=None):
        def beside(phase, top):
            return () if during is None else (during(phase, top),)

        x0 = lax.ppermute(up, "gx", route("gx", 1))
        x1 = lax.ppermute(down, "gx", route("gx", -1))
        waits = beside(0, top)
        up, down, top = self.y_packer(len(waits))(own, top, x0, x1, *waits)
        y0 = lax.ppermute(up, "gy", route("gy", 1))
        y1 = lax.ppermute(down, "gy", route("gy", -1))
        waits = beside(1, top)
        *messages, top = self.z_packer(len(waits))(own, top, x0, x1, y0, y1, *waits)
        z = [lax.ppermute(m, "gz", route("gz", d)) for m, d in zip(messages, (1, -1))]
        beside(2, top)
        return (own, top, x0, x1, y0, y1, *z)

    def lay_out(self, halo, own, x0, x1, y0, y1, z):
        self.put_own(halo, own)
        self.put_x(halo, x0, x1)
        self.put_y(halo, y0, y1)
        self.put_z(halo, z)

    def latest_top(self, top, z):
        return self.largest(top, self.z_faces * self.z_rows, z)


def rounded(x):
    return x.astype(jnp.bfloat16).astype(jnp.float32)


def split3(x):
    a = rounded(x)
    b = rounded(x - a)
    return a, b, x - a - b


def start_kernel(s):
    faces = Faces(s, FIELDS)

    def body(counts_in, placements_in, mass_in, temp_in, own, top_out, up, down,
             counts, placements, mass, temp, arrived):
        copies = [
            pltpu.make_async_copy(a, b, arrived.at[k])
            for k, (a, b) in enumerate(
                ((counts_in, counts), (placements_in, placements), (mass_in, mass), (temp_in, temp))
            )
        ]
        for copy in copies:
            copy.start()
        for copy in copies:
            copy.wait()
        slot = lax.broadcasted_iota(jnp.int32, (1, s.slots), 1)
        for x in range(s.nx):
            for y in range(s.ny):
                start = (x * s.ny + y) * s.nz
                for d in range(3):
                    own[d * s.cells + start : d * s.cells + start + s.nz, :] = placements[d, x, y]
                rows = [
                    jnp.where(slot < counts[x, y, z], mass[x, y, z : z + 1, :], 0.0) for z in range(s.nz)
                ]
                own[3 * s.cells + start : 3 * s.cells + start + s.nz, :] = jnp.concatenate(rows, axis=0)
                own[4 * s.cells + start : 4 * s.cells + start + s.nz, :] = temp[x, y]
        none = jnp.zeros((1, s.slots), jnp.float32)
        top_out[...] = none
        faces.pack_x(own, none, up, down)

    block = (s.nx, s.ny, s.nz, s.slots)
    return pl.pallas_call(
        body,
        in_specs=[pl.BlockSpec(memory_space=pltpu.HBM)] * 4,
        out_shape=(f32(FIELDS * s.cells, s.slots), f32(1, s.slots), *faces.x_messages()),
        scratch_shapes=[
            pltpu.SMEM(block[:3], jnp.int32),
            pltpu.VMEM((3, *block), jnp.float32),
            pltpu.VMEM(block, jnp.float32),
            pltpu.VMEM(block, jnp.float32),
            pltpu.SemaphoreType.DMA((4,)),
        ],
        compiler_params=SMALL,
        name="start",
    )


def source_rows(s, volume, scaled, temp, gains):
    row = lax.broadcasted_iota(jnp.int32, (8, s.slots), 0)
    use_c = (row % 4) < 2
    use_u = row < 4
    odd = (row % 2) == 1

    def one(cell, carry):
        def rows(ref):
            return jnp.broadcast_to(ref[pl.ds(cell, 1), :], (8, s.slots))

        full = jnp.where(use_c, rows(scaled), rows(volume)) * jnp.where(use_u, rows(temp), 1.0)
        top = rounded(full)
        gains[cell] = jnp.where(odd, full - top, top)
        return carry

    lax.fori_loop(0, s.padded, one, 0, unroll=6)


def gain_pair(gains, cell):
    return jnp.concatenate([gains[cell], gains[cell + 1]], axis=0).astype(jnp.bfloat16)


def add_sums(s, total, cell, sums):
    for k in range(2):
        rows = pl.ds(pl.multiple_of((cell + k) * 8, 8), 8)
        sums[rows, :] = sums[rows, :] + total[8 * k : 8 * k + 8, k * s.slots : (k + 1) * s.slots]


def flow_of(s, sums, conduct_own, temp_own):
    def of(r):
        return sums[pl.ds(r, s.cells, stride=8), :]

    weight = of(4) + of(5) + conduct_own * (of(6) + of(7))
    flow = of(0) + of(1) + conduct_own * (of(2) + of(3)) - temp_own * weight
    return flow, weight


def line(s, c):
    own = combos_x(s)
    x, side = (c + 1) // 3, c - own
    return (
        jnp.where(c < own, x, side * (s.nx - 1)),
        jnp.where(c < own, c - 2 * x + 1, side * (s.px - 1)),
    )


def apply_line(s, c, yz, gains, kernel, sums):
    x, source_x = line(s, c)
    y, zp = yz // s.half, yz % s.half
    parts = [
        gain_pair(gains, (source_x * s.py + y + j) * s.pz + 2 * zp + e) for j in range(3) for e in range(3)
    ]
    total = jnp.dot(jnp.concatenate(parts, axis=1), kernel[c, yz], preferred_element_type=jnp.float32)
    add_sums(s, total, 2 * (x * s.ny * s.half + yz), sums)


def kernel_shape(s):
    return jax.ShapeDtypeStruct((combos_x(s) + 2, s.ny * s.half, 9 * s.slots, 2 * s.slots), jnp.bfloat16)


def conductivity(temp):
    return temp * temp * jnp.sqrt(temp)


def rows_of(s, k, ref, cell):
    return jnp.broadcast_to(ref[k, pl.ds(cell, 1), :], (8, s.slots))


def on_grid(ref, d, count):
    return (ref[d * count : (d + 1) * count, :] - 0.5 + ROUNDER) - ROUNDER


def source_tables(s, ref, count, halves):
    square = 0.0
    for d in range(3):
        q = on_grid(ref, d, count)
        halves[2 * d] = rounded(q)
        halves[2 * d + 1] = q - rounded(q)
        square = square + q * q
    for d, part in enumerate(split3(square)):
        halves[6 + d] = part


def source_quads(s, halves, first_cell, present, left, at):
    row = lax.broadcasted_iota(jnp.int32, (8, s.slots), 0)
    zero8 = jnp.zeros((8, s.slots), jnp.float32)
    blocks = []
    for z in range(s.pz):
        if z not in present:
            blocks += [zero8] * 4
            continue
        cell = first_cell + present.index(z)
        for d in range(3):
            block = jnp.where(row % 2 == 0, rows_of(s, 2 * d, halves, cell), rows_of(s, 2 * d + 1, halves, cell))
            rest = jnp.where(row < 7, 1.0, rows_of(s, 6 + d, halves, cell))
            blocks.append(jnp.where(row < 4, block, rest))
        blocks.append(zero8)
    for zp in range(s.half):
        quad = jnp.concatenate(blocks[8 * zp : 8 * zp + 16], axis=0)
        left[at * s.half + zp] = quad.T.astype(jnp.bfloat16)


def target_tables(s, own, targets):
    for d in range(3):
        q = on_grid(own, d, s.cells)
        for k, shift in enumerate(SHIFTS):
            t = q - float(shift)
            h = rounded(t)
            for r, part in enumerate((-2.0 * h, -2.0 * (t - h), *split3(t * t))):
                targets[(d * 3 + k) * 5 + r] = part


def target_blocks(s, targets, cell, low, high):
    row = lax.broadcasted_iota(jnp.int32, (8, s.slots), 0)
    rows = []
    for d in range(3):
        for k in range(3):
            part = [rows_of(s, (d * 3 + k) * 5 + r, targets, cell) for r in range(5)]
            block = jnp.where(row == 5, part[3], jnp.where(row == 6, part[4], 1.0))
            block = jnp.where(row < 4, part[1], jnp.where(row == 4, part[2], block))
            rows.append(jnp.where(row < 2, part[0], block))
    for i in range(3):
        for j in range(3):
            low[cell * 9 + i * 3 + j] = jnp.concatenate([rows[i], rows[3 + j]], 0).astype(jnp.bfloat16)
    for e in range(3):
        high[cell * 3 + e] = jnp.concatenate([rows[6 + e], jnp.zeros_like(rows[0])], 0).astype(jnp.bfloat16)


def pair_block(s, c, yz, cell, i, j, e, source, low, high, kernel):
    nothing = jnp.zeros((16, s.slots), jnp.bfloat16)
    lanes = []
    for k in range(2):
        parts = [nothing] * 8
        parts[2 * (e + k)] = low[(cell + k) * 9 + i * 3 + j]
        parts[2 * (e + k) + 1] = high[(cell + k) * 3 + e]
        lanes.append(jnp.concatenate(parts, axis=0))
    right = jnp.concatenate(lanes, axis=1)
    dist = jnp.dot(source, right, preferred_element_type=jnp.float32)
    gap = 1.0 - dist * lax.rsqrt(jnp.maximum(dist, 2.5e-7))
    value = jnp.maximum((gap * gap * gap).astype(jnp.bfloat16), jnp.bfloat16(0.0))
    kernel[c, yz, (j * 3 + e) * s.slots : (j * 3 + e + 1) * s.slots, :] = value


def inner_z(s, zp, e):
    return 0 <= 2 * zp + e - 1 and 2 * zp + e < s.nz


def combos_x(s):
    return 3 * s.nx - 2


def inner_kernel(s, room, begin, end):
    slots = s.slots
    opening = begin == 0

    def blocks(left, low, high, kernel):
        def along_x(c, carry):
            x, source_x = line(s, c)
            for yz in range(s.ny * s.half):
                y, zp = yz // s.half, yz % s.half
                cell = 2 * (x * s.ny * s.half + yz)
                for j in range(3):
                    if not 0 <= y + j - 1 < s.ny:
                        continue
                    source = left[((source_x - 1) * s.ny + y + j - 1) * s.half + zp]
                    for e in range(3):
                        if inner_z(s, zp, e):
                            pair_block(s, c, yz, cell, source_x - x, j, e, source, low, high, kernel)
            return carry

        lax.fori_loop(begin, end, along_x, 0)

    def first(own, after, kernel, low, high, left, done, halves, targets):
        done[...] = after[...]
        source_tables(s, own, s.cells, halves)
        target_tables(s, own, targets)

        def prepare(column, carry):
            source_quads(s, halves, column * s.nz, list(range(1, s.nz + 1)), left, column)
            for z in range(s.nz):
                target_blocks(s, targets, column * s.nz + z, low, high)
            return carry

        lax.fori_loop(0, s.nx * s.ny, prepare, 0)
        blocks(left, low, high, kernel)

    def second(kernel_in, low, high, left, after, kernel, done):
        done[...] = after[...]
        blocks(left, low, high, kernel)

    kernel = kernel_shape(s)
    if opening:
        return pl.pallas_call(
            first,
            out_shape=(
                kernel,
                jax.ShapeDtypeStruct((s.cells * 9, 16, slots), jnp.bfloat16),
                jax.ShapeDtypeStruct((s.cells * 3, 16, slots), jnp.bfloat16),
                jax.ShapeDtypeStruct((s.pairs, slots, 128), jnp.bfloat16),
                f32(1, slots),
            ),
            scratch_shapes=[
                pltpu.VMEM((9, s.cells, slots), jnp.float32),
                pltpu.VMEM((45, s.cells, slots), jnp.float32),
            ],
            compiler_params=pltpu.CompilerParams(vmem_limit_bytes=room),
            name="inner_first",
        )
    return pl.pallas_call(
        second,
        out_shape=(kernel, f32(1, slots)),
        input_output_aliases={0: 0},
        compiler_params=pltpu.CompilerParams(vmem_limit_bytes=room),
        name="inner_second",
    )


def outer_kernel(s, room):
    slots = s.slots
    fields = Faces(s, FIELDS)
    faces = Faces(s, 1)
    arrivals = len(fields.z_messages())

    def body(kernel_in, low, high, own, x0, x1, y0, y1, *rest):
        z, rest = rest[:arrivals], rest[arrivals:]
        (kernel, flow_out, volume_out, scaled_out, conduct_own, temp_own, top_out, up, down,
         halo, left, gains, sums, halves) = rest
        fields.lay_out(halo, own, x0, x1, y0, y1, z)
        temp = halo.at[pl.ds(4 * s.padded, s.padded)]
        volume_out[...] = halo[3 * s.padded : 4 * s.padded, :]
        scaled_out[...] = volume_out[...] * conductivity(temp[...])
        temp_own[...] = own[4 * s.cells : 5 * s.cells, :]
        conduct_own[...] = conductivity(temp_own[...])
        source_rows(s, volume_out, scaled_out, temp, gains)
        source_tables(s, halo, s.padded, halves)

        def features(column, carry):
            source_quads(s, halves, column * s.pz, list(range(s.pz)), left, column)
            return carry

        lax.fori_loop(0, s.columns, features, 0, unroll=5)

        sums[...] = jnp.zeros_like(sums)

        def along_x(skip, c, carry):
            x, source_x = line(s, c)
            for yz in range(s.ny * s.half):
                y, zp = yz // s.half, yz % s.half
                cell = 2 * (x * s.ny * s.half + yz)
                for j in range(3):
                    inside = skip and 0 <= y + j - 1 < s.ny
                    source = left[(source_x * s.py + y + j) * s.half + zp]
                    for e in range(3):
                        if not (inside and inner_z(s, zp, e)):
                            pair_block(s, c, yz, cell, source_x - x, j, e, source, low, high, kernel)
                if yz > 0:
                    apply_line(s, c, yz - 1, gains, kernel, sums)
            apply_line(s, c, s.ny * s.half - 1, gains, kernel, sums)
            return carry

        lax.fori_loop(0, combos_x(s), functools.partial(along_x, True), 0)
        lax.fori_loop(combos_x(s), combos_x(s) + 2, functools.partial(along_x, False), 0)

        flow, weight = flow_of(s, sums, conduct_own[...], temp_own[...])
        flow_out[...] = flow
        occupied = own[3 * s.cells : 4 * s.cells, :] > 0.0
        top = jnp.max(jnp.where(occupied, weight, 0.0), axis=0, keepdims=True)
        top_out[...] = top
        faces.pack_x(flow_out, top, up, down)

    cells, padded = f32(s.cells, slots), f32(s.padded, slots)
    return pl.pallas_call(
        body,
        out_shape=(
            kernel_shape(s),
            cells,
            padded,
            padded,
            cells,
            cells,
            f32(1, slots),
            *faces.x_messages(),
        ),
        input_output_aliases={0: 0},
        scratch_shapes=[
            fields.halo_shape,
            pltpu.VMEM((s.columns * s.half, slots, 128), jnp.bfloat16),
            pltpu.VMEM((s.padded, 8, slots), jnp.float32),
            pltpu.VMEM((s.cells * 8, slots), jnp.float32),
            pltpu.VMEM((9, s.padded, slots), jnp.float32),
        ],
        compiler_params=pltpu.CompilerParams(vmem_limit_bytes=room),
        name="outer_and_first_flow",
    )


def next_kernel(s, room, last):
    slots = s.slots
    faces = Faces(s, 1)
    arrivals = len(faces.z_messages())

    def body(kernel, volume, scaled, conduct_own, *rest):
        if last:
            temp_own, flow1, *rest = rest
        own, top, x0, x1, y0, y1, *rest = rest
        z, rest = rest[:arrivals], rest[arrivals:]
        if last:
            out, temp, gains, sums, *rest = rest
        else:
            flow_out, top_out, up, down, temp, gains, sums = rest
        faces.lay_out(temp, own, x0, x1, y0, y1, z)
        most = faces.latest_top(top, z)
        source_rows(s, volume, scaled, temp, gains)

        sums[...] = jnp.zeros_like(sums)

        def along_x(c, carry):
            for yz in range(s.ny * s.half):
                apply_line(s, c, yz, gains, kernel, sums)
            return carry

        lax.fori_loop(0, combos_x(s) + 2, along_x, 0, unroll=3)
        flow, _ = flow_of(s, sums, conduct_own[...], own[...])
        if last and covered():
            rows, block, arrived = rest
            step = step_factor / jnp.max(most, axis=1, keepdims=True)
            rows[...] = polynomial(temp_own[...], step, flow1[...], own[...], flow)
            for x in range(s.nx):
                for y in range(s.ny):
                    start = (x * s.ny + y) * s.nz
                    block[x, y] = rows[start : start + s.nz, :]
            copy = pltpu.make_async_copy(block, out, arrived)
            copy.start()
            copy.wait()
        elif last:
            out[...] = flow
        else:
            flow_out[...] = flow
            top_out[...] = most
            faces.pack_x(flow_out, most, up, down)

    cells, shape = f32(s.cells, slots), (s.nx, s.ny, s.nz, slots)
    outs = (cells, f32(1, slots), *faces.x_messages())
    spaces = [pltpu.VMEM] * len(outs)
    scratch = [
        faces.halo_shape,
        pltpu.VMEM((s.padded, 8, slots), jnp.float32),
        pltpu.VMEM((s.cells * 8, slots), jnp.float32),
    ]
    if last and covered():
        outs, spaces = (f32(*shape),), [pl.ANY]
        scratch += [pltpu.VMEM((s.cells, slots), jnp.float32), pltpu.VMEM(shape, jnp.float32), pltpu.SemaphoreType.DMA]
    elif last:
        outs, spaces = (cells,), [pltpu.VMEM]
    return pl.pallas_call(
        body,
        out_shape=outs,
        out_specs=tuple(pl.BlockSpec(memory_space=space) for space in spaces),
        scratch_shapes=scratch,
        compiler_params=pltpu.CompilerParams(vmem_limit_bytes=room),
        name="last_flow" if last else "next_flow",
    )


def covered():
    return all(lax.axis_size(axis) <= 5 for axis in AXES)


def polynomial(start, step, flow1, flow2, flow3):
    return start + step * (flow1 + step * (0.5 * flow2 + step * (1.0 / 15.0) * flow3))


def local(relative_placements, mass_per_density, opening_heat_level, bin_fill_counts):
    nx, ny, nz, slots = opening_heat_level.shape
    s = Sizes(nx, ny, nz, slots)
    fields, faces = Faces(s, FIELDS), Faces(s, 1)
    arguments = (bin_fill_counts, relative_placements, mass_per_density, opening_heat_level)
    started = start_kernel(s)(*[pltpu.with_memory_space_constraint(a, pltpu.HBM) for a in arguments])
    made = []
    own_bytes = 4 * slots * rounded_up(FIELDS * s.cells)
    parts = (0, 2 * combos_x(s) // 7, 5 * combos_x(s) // 7, combos_x(s))

    def during(phase, after):
        begin, end = parts[phase], parts[phase + 1]
        if phase == 0:
            *outs, done = inner_kernel(s, ROOM - own_bytes - 4096, begin, end)(started[0], after)
            made.extend(outs)
        else:
            made[0], done = inner_kernel(s, ROOM, begin, end)(*made, after)
        return done

    own, _, *messages = fields.exchange(*started, during)
    kernel, low, high, _ = made
    kernel, flow1, volume, scaled, conduct_own, temp_own, top, up, down = outer_kernel(s, ROOM - own_bytes)(
        kernel, low, high, own, *messages
    )
    arrived = faces.exchange(flow1, top, up, down)
    flow2, top, up, down = next_kernel(s, ROOM, False)(kernel, volume, scaled, conduct_own, *arrived)
    arrived = faces.exchange(flow2, top, up, down)
    (final,) = next_kernel(s, ROOM, True)(kernel, volume, scaled, conduct_own, temp_own, flow1, *arrived)
    if not covered():
        top, flow3 = lax.optimization_barrier((arrived[1], final))
        step = step_factor / lax.pmax(jnp.max(top), AXES)
        final = polynomial(temp_own, step, flow1, flow2, flow3).reshape(nx, ny, nz, slots)
    return final


def solution(mesh):
    in_specs = (
        P(None, "gx", "gy", "gz", None),
        P("gx", "gy", "gz", None),
        P("gx", "gy", "gz", None),
        P("gx", "gy", "gz"),
    )
    out_specs = P("gx", "gy", "gz", None)
    return jax.shard_map(local, mesh=mesh, in_specs=in_specs, out_specs=out_specs, check_vma=False)
```

```python
import functools

import jax
import jax.numpy as jnp
from jax import lax
from jax.experimental import pallas as pl
from jax.experimental.pallas import tpu as pltpu
from jax.sharding import PartitionSpec as P

step_factor = 2.0
AXES = ("gx", "gy", "gz")
ROUNDER = 192.0
SHIFTS = (-1, 0, 1)
FIELDS = 5
ROOM = 8 << 20
SMALL = pltpu.CompilerParams(vmem_limit_bytes=2 << 20)


def route(axis, distance):
    size = lax.axis_size(axis)
    return [(i, (i + distance) % size) for i in range(size)]


def rounded_up(rows):
    return -(-rows // 8) * 8


def f32(*shape):
    return jax.ShapeDtypeStruct(shape, jnp.float32)


class Sizes:
    def __init__(self, nx, ny, nz, slots):
        self.nx, self.ny, self.nz, self.slots = nx, ny, nz, slots
        self.px, self.py, self.pz = nx + 2, ny + 2, nz + 2
        self.cells = nx * ny * nz
        self.padded = self.px * self.py * self.pz
        self.half = nz // 2
        self.pairs = nx * ny * self.half
        self.columns = self.px * self.py


class Faces:
    def __init__(self, s, fields):
        self.s, self.fields = s, fields
        self.x_rows = s.ny * s.nz
        self.y_rows = s.px * s.nz
        self.joined = lax.axis_size("gz") == 2
        self.z_rows = s.px * s.py
        self.z_faces = 2 if self.joined else 1
        self.halo_shape = pltpu.VMEM((fields * s.padded, s.slots), jnp.float32)

    def message(self, rows):
        return f32(rounded_up(self.fields * rows + 1), self.s.slots)

    def x_messages(self):
        return (self.message(self.x_rows),) * 2

    def y_messages(self):
        return (self.message(self.y_rows),) * 2

    def z_messages(self):
        return (self.message(self.z_faces * self.z_rows),) * (2 // self.z_faces)

    def row(self, f, x, y, z):
        return f * self.s.padded + (x * self.s.py + y) * self.s.pz + z

    def put_own(self, halo, own):
        s = self.s
        for f in range(self.fields):
            for x in range(s.nx):
                for y in range(s.ny):
                    at, start = self.row(f, x + 1, y + 1, 1), f * s.cells + (x * s.ny + y) * s.nz
                    halo[at : at + s.nz, :] = own[start : start + s.nz, :]

    def put_x(self, halo, before, after):
        s = self.s
        for f in range(self.fields):
            for side, x in ((before, 0), (after, s.nx + 1)):
                for y in range(s.ny):
                    at, start = self.row(f, x, y + 1, 1), f * self.x_rows + y * s.nz
                    halo[at : at + s.nz, :] = side[start : start + s.nz, :]

    def put_y(self, halo, before, after):
        s = self.s
        for f in range(self.fields):
            for side, y in ((before, 0), (after, s.ny + 1)):
                for x in range(s.px):
                    at, start = self.row(f, x, y, 1), f * self.y_rows + x * s.nz
                    halo[at : at + s.nz, :] = side[start : start + s.nz, :]

    def z_places(self, below, above):
        for f in range(self.fields):
            for k, z in ((0, below), (1, above)):
                m, base = (0, k * self.z_rows) if self.joined else (k, 0)
                for column in range(self.z_rows):
                    yield m, f * self.z_faces * self.z_rows + base + column, f, column, z

    def put_z(self, halo, sides):
        for m, start, f, column, z in self.z_places(0, self.s.nz + 1):
            at = f * self.s.padded + column * self.s.pz + z
            halo[at : at + 1, :] = sides[m][start : start + 1, :]

    def end(self, message, rows, top):
        n = self.fields * rows
        message[n : n + 1, :] = top

    def pack_x(self, own, top, up, down):
        s = self.s
        n = self.x_rows
        for f in range(self.fields):
            up[f * n : f * n + n, :] = own[f * s.cells + (s.nx - 1) * n : f * s.cells + s.nx * n, :]
            down[f * n : f * n + n, :] = own[f * s.cells : f * s.cells + n, :]
        for m in (up, down):
            self.end(m, n, top)

    def pack_y(self, halo, top, up, down):
        s = self.s
        for f in range(self.fields):
            for x in range(s.px):
                for m, y in ((up, s.ny), (down, 1)):
                    at, start = self.row(f, x, y, 1), f * self.y_rows + x * s.nz
                    m[start : start + s.nz, :] = halo[at : at + s.nz, :]
        for m in (up, down):
            self.end(m, self.y_rows, top)

    def pack_z(self, halo, top, messages):
        for m, start, f, column, z in self.z_places(self.s.nz, 1):
            at = f * self.s.padded + column * self.s.pz + z
            messages[m][start : start + 1, :] = halo[at : at + 1, :]
        for m in messages:
            self.end(m, self.z_faces * self.z_rows, top)

    def largest(self, top, rows, refs):
        n = self.fields * rows
        return jnp.maximum(top[...], jnp.maximum(refs[0][n : n + 1, :], refs[-1][n : n + 1, :]))

    def y_packer(self, waits):
        def body(own, top, before, after, *rest):
            up, down, top_out, halo = rest[waits:]
            self.put_own(halo, own)
            self.put_x(halo, before, after)
            most = self.largest(top, self.x_rows, (before, after))
            top_out[...] = most
            self.pack_y(halo, most, up, down)

        return pl.pallas_call(
            body,
            out_shape=(*self.y_messages(), f32(1, self.s.slots)),
            scratch_shapes=[self.halo_shape],
            compiler_params=SMALL,
            name="pack_y",
        )

    def z_packer(self, waits):
        count = len(self.z_messages())

        def body(own, top, x0, x1, y0, y1, *rest):
            rest = rest[waits:]
            messages, top_out, halo = rest[:count], rest[count], rest[-1]
            self.put_own(halo, own)
            self.put_x(halo, x0, x1)
            self.put_y(halo, y0, y1)
            most = self.largest(top, self.y_rows, (y0, y1))
            top_out[...] = most
            self.pack_z(halo, most, messages)

        return pl.pallas_call(
            body,
            out_shape=(*self.z_messages(), f32(1, self.s.slots)),
            scratch_shapes=[self.halo_shape],
            compiler_params=SMALL,
            name="pack_z",
        )

    def exchange(self, own, top, up, down, during=None):
        def beside(phase, top):
            return () if during is None else (during(phase, top),)

        x0 = lax.ppermute(up, "gx", route("gx", 1))
        x1 = lax.ppermute(down, "gx", route("gx", -1))
        waits = beside(0, top)
        up, down, top = self.y_packer(len(waits))(own, top, x0, x1, *waits)
        y0 = lax.ppermute(up, "gy", route("gy", 1))
        y1 = lax.ppermute(down, "gy", route("gy", -1))
        waits = beside(1, top)
        *messages, top = self.z_packer(len(waits))(own, top, x0, x1, y0, y1, *waits)
        z = [lax.ppermute(m, "gz", route("gz", d)) for m, d in zip(messages, (1, -1))]
        beside(2, top)
        return (own, top, x0, x1, y0, y1, *z)

    def lay_out(self, halo, own, x0, x1, y0, y1, z):
        self.put_own(halo, own)
        self.put_x(halo, x0, x1)
        self.put_y(halo, y0, y1)
        self.put_z(halo, z)

    def latest_top(self, top, z):
        return self.largest(top, self.z_faces * self.z_rows, z)


def rounded(x):
    return x.astype(jnp.bfloat16).astype(jnp.float32)


def split3(x):
    a = rounded(x)
    b = rounded(x - a)
    return a, b, x - a - b


def start_kernel(s):
    faces = Faces(s, FIELDS)

    def body(counts_in, placements_in, mass_in, temp_in, own, top_out, up, down,
             counts, placements, mass, temp, arrived):
        copies = [
            pltpu.make_async_copy(a, b, arrived.at[k])
            for k, (a, b) in enumerate(
                ((counts_in, counts), (placements_in, placements), (mass_in, mass), (temp_in, temp))
            )
        ]
        for copy in copies:
            copy.start()
        for copy in copies:
            copy.wait()
        slot = lax.broadcasted_iota(jnp.int32, (1, s.slots), 1)
        for x in range(s.nx):
            for y in range(s.ny):
                start = (x * s.ny + y) * s.nz
                for d in range(3):
                    own[d * s.cells + start : d * s.cells + start + s.nz, :] = placements[d, x, y]
                rows = [
                    jnp.where(slot < counts[x, y, z], mass[x, y, z : z + 1, :], 0.0) for z in range(s.nz)
                ]
                own[3 * s.cells + start : 3 * s.cells + start + s.nz, :] = jnp.concatenate(rows, axis=0)
                own[4 * s.cells + start : 4 * s.cells + start + s.nz, :] = temp[x, y]
        none = jnp.zeros((1, s.slots), jnp.float32)
        top_out[...] = none
        faces.pack_x(own, none, up, down)

    block = (s.nx, s.ny, s.nz, s.slots)
    return pl.pallas_call(
        body,
        in_specs=[pl.BlockSpec(memory_space=pltpu.HBM)] * 4,
        out_shape=(f32(FIELDS * s.cells, s.slots), f32(1, s.slots), *faces.x_messages()),
        scratch_shapes=[
            pltpu.SMEM(block[:3], jnp.int32),
            pltpu.VMEM((3, *block), jnp.float32),
            pltpu.VMEM(block, jnp.float32),
            pltpu.VMEM(block, jnp.float32),
            pltpu.SemaphoreType.DMA((4,)),
        ],
        compiler_params=SMALL,
        name="start",
    )


def source_rows(s, volume, scaled, temp, gains):
    row = lax.broadcasted_iota(jnp.int32, (8, s.slots), 0)
    use_c = (row % 4) < 2
    use_u = row < 4
    odd = (row % 2) == 1

    def one(cell, carry):
        def rows(ref):
            return jnp.broadcast_to(ref[pl.ds(cell, 1), :], (8, s.slots))

        full = jnp.where(use_c, rows(scaled), rows(volume)) * jnp.where(use_u, rows(temp), 1.0)
        top = rounded(full)
        gains[cell] = jnp.where(odd, full - top, top)
        return carry

    lax.fori_loop(0, s.padded, one, 0, unroll=6)


def gain_pair(gains, cell):
    return jnp.concatenate([gains[cell], gains[cell + 1]], axis=0).astype(jnp.bfloat16)


def add_sums(s, total, cell, sums):
    for k in range(2):
        rows = pl.ds(pl.multiple_of((cell + k) * 8, 8), 8)
        sums[rows, :] = sums[rows, :] + total[8 * k : 8 * k + 8, k * s.slots : (k + 1) * s.slots]


def flow_of(s, sums, conduct_own, temp_own):
    def of(r):
        return sums[pl.ds(r, s.cells, stride=8), :]

    weight = of(4) + of(5) + conduct_own * (of(6) + of(7))
    flow = of(0) + of(1) + conduct_own * (of(2) + of(3)) - temp_own * weight
    return flow, weight


def line(s, c):
    own = combos_x(s)
    x, side = (c + 1) // 3, c - own
    return (
        jnp.where(c < own, x, side * (s.nx - 1)),
        jnp.where(c < own, c - 2 * x + 1, side * (s.px - 1)),
    )


def apply_line(s, c, yz, gains, kernel, sums):
    x, source_x = line(s, c)
    y, zp = yz // s.half, yz % s.half
    parts = [
        gain_pair(gains, (source_x * s.py + y + j) * s.pz + 2 * zp + e) for j in range(3) for e in range(3)
    ]
    total = jnp.dot(jnp.concatenate(parts, axis=1), kernel[c, yz], preferred_element_type=jnp.float32)
    add_sums(s, total, 2 * (x * s.ny * s.half + yz), sums)


def kernel_shape(s):
    return jax.ShapeDtypeStruct((combos_x(s) + 2, s.ny * s.half, 9 * s.slots, 2 * s.slots), jnp.bfloat16)


def conductivity(temp):
    return temp * temp * jnp.sqrt(temp)


def rows_of(s, k, ref, cell):
    return jnp.broadcast_to(ref[k, pl.ds(cell, 1), :], (8, s.slots))


def on_grid(ref, d, count):
    return (ref[d * count : (d + 1) * count, :] - 0.5 + ROUNDER) - ROUNDER


def source_tables(s, ref, count, halves):
    square = 0.0
    for d in range(3):
        q = on_grid(ref, d, count)
        halves[2 * d] = rounded(q)
        halves[2 * d + 1] = q - rounded(q)
        square = square + q * q
    for d, part in enumerate(split3(square)):
        halves[6 + d] = part


def source_quads(s, halves, first_cell, present, left, at):
    row = lax.broadcasted_iota(jnp.int32, (8, s.slots), 0)
    zero8 = jnp.zeros((8, s.slots), jnp.float32)
    blocks = []
    for z in range(s.pz):
        if z not in present:
            blocks += [zero8] * 4
            continue
        cell = first_cell + present.index(z)
        for d in range(3):
            block = jnp.where(row % 2 == 0, rows_of(s, 2 * d, halves, cell), rows_of(s, 2 * d + 1, halves, cell))
            rest = jnp.where(row < 7, 1.0, rows_of(s, 6 + d, halves, cell))
            blocks.append(jnp.where(row < 4, block, rest))
        blocks.append(zero8)
    for zp in range(s.half):
        quad = jnp.concatenate(blocks[8 * zp : 8 * zp + 16], axis=0)
        left[at * s.half + zp] = quad.T.astype(jnp.bfloat16)


def target_tables(s, own, targets):
    for d in range(3):
        q = on_grid(own, d, s.cells)
        for k, shift in enumerate(SHIFTS):
            t = q - float(shift)
            h = rounded(t)
            for r, part in enumerate((-2.0 * h, -2.0 * (t - h), *split3(t * t))):
                targets[(d * 3 + k) * 5 + r] = part


def target_blocks(s, targets, cell, low, high):
    row = lax.broadcasted_iota(jnp.int32, (8, s.slots), 0)
    rows = []
    for d in range(3):
        for k in range(3):
            part = [rows_of(s, (d * 3 + k) * 5 + r, targets, cell) for r in range(5)]
            block = jnp.where(row == 5, part[3], jnp.where(row == 6, part[4], 1.0))
            block = jnp.where(row < 4, part[1], jnp.where(row == 4, part[2], block))
            rows.append(jnp.where(row < 2, part[0], block))
    for i in range(3):
        for j in range(3):
            low[cell * 9 + i * 3 + j] = jnp.concatenate([rows[i], rows[3 + j]], 0).astype(jnp.bfloat16)
    for e in range(3):
        high[cell * 3 + e] = jnp.concatenate([rows[6 + e], jnp.zeros_like(rows[0])], 0).astype(jnp.bfloat16)


def pair_block(s, c, yz, cell, i, j, e, source, low, high, kernel):
    nothing = jnp.zeros((16, s.slots), jnp.bfloat16)
    lanes = []
    for k in range(2):
        parts = [nothing] * 8
        parts[2 * (e + k)] = low[(cell + k) * 9 + i * 3 + j]
        parts[2 * (e + k) + 1] = high[(cell + k) * 3 + e]
        lanes.append(jnp.concatenate(parts, axis=0))
    right = jnp.concatenate(lanes, axis=1)
    dist = jnp.dot(source, right, preferred_element_type=jnp.float32)
    gap = 1.0 - dist * lax.rsqrt(jnp.maximum(dist, 2.5e-7))
    value = jnp.maximum((gap * gap * gap).astype(jnp.bfloat16), jnp.bfloat16(0.0))
    kernel[c, yz, (j * 3 + e) * s.slots : (j * 3 + e + 1) * s.slots, :] = value


def inner_z(s, zp, e):
    return 0 <= 2 * zp + e - 1 and 2 * zp + e < s.nz


def combos_x(s):
    return 3 * s.nx - 2


def inner_kernel(s, room, begin, end):
    slots = s.slots
    opening = begin == 0

    def blocks(left, low, high, kernel):
        def along_x(c, carry):
            x, source_x = line(s, c)
            for yz in range(s.ny * s.half):
                y, zp = yz // s.half, yz % s.half
                cell = 2 * (x * s.ny * s.half + yz)
                for j in range(3):
                    if not 0 <= y + j - 1 < s.ny:
                        continue
                    source = left[((source_x - 1) * s.ny + y + j - 1) * s.half + zp]
                    for e in range(3):
                        if inner_z(s, zp, e):
                            pair_block(s, c, yz, cell, source_x - x, j, e, source, low, high, kernel)
            return carry

        lax.fori_loop(begin, end, along_x, 0, unroll=True)

    def first(own, after, kernel, low, high, left, done, halves, targets):
        done[...] = after[...]
        source_tables(s, own, s.cells, halves)
        target_tables(s, own, targets)

        def prepare(column, carry):
            source_quads(s, halves, column * s.nz, list(range(1, s.nz + 1)), left, column)
            for z in range(s.nz):
                target_blocks(s, targets, column * s.nz + z, low, high)
            return carry

        lax.fori_loop(0, s.nx * s.ny, prepare, 0)
        blocks(left, low, high, kernel)

    def second(kernel_in, low, high, left, after, kernel, done):
        done[...] = after[...]
        blocks(left, low, high, kernel)

    kernel = kernel_shape(s)
    if opening:
        return pl.pallas_call(
            first,
            out_shape=(
                kernel,
                jax.ShapeDtypeStruct((s.cells * 9, 16, slots), jnp.bfloat16),
                jax.ShapeDtypeStruct((s.cells * 3, 16, slots), jnp.bfloat16),
                jax.ShapeDtypeStruct((s.pairs, slots, 128), jnp.bfloat16),
                f32(1, slots),
            ),
            scratch_shapes=[
                pltpu.VMEM((9, s.cells, slots), jnp.float32),
                pltpu.VMEM((45, s.cells, slots), jnp.float32),
            ],
            compiler_params=pltpu.CompilerParams(vmem_limit_bytes=room),
            name="inner_first",
        )
    return pl.pallas_call(
        second,
        out_shape=(kernel, f32(1, slots)),
        input_output_aliases={0: 0},
        compiler_params=pltpu.CompilerParams(vmem_limit_bytes=room),
        name="inner_second",
    )


def outer_kernel(s, room):
    slots = s.slots
    fields = Faces(s, FIELDS)
    faces = Faces(s, 1)
    arrivals = len(fields.z_messages())

    def body(kernel_in, low, high, own, x0, x1, y0, y1, *rest):
        z, rest = rest[:arrivals], rest[arrivals:]
        (kernel, flow_out, volume_out, scaled_out, conduct_own, temp_own, top_out, up, down,
         halo, left, gains, sums, halves) = rest
        fields.lay_out(halo, own, x0, x1, y0, y1, z)
        temp = halo.at[pl.ds(4 * s.padded, s.padded)]
        volume_out[...] = halo[3 * s.padded : 4 * s.padded, :]
        scaled_out[...] = volume_out[...] * conductivity(temp[...])
        temp_own[...] = own[4 * s.cells : 5 * s.cells, :]
        conduct_own[...] = conductivity(temp_own[...])
        source_rows(s, volume_out, scaled_out, temp, gains)
        source_tables(s, halo, s.padded, halves)

        def features(column, carry):
            source_quads(s, halves, column * s.pz, list(range(s.pz)), left, column)
            return carry

        lax.fori_loop(0, s.columns, features, 0, unroll=5)

        sums[...] = jnp.zeros_like(sums)

        def along_x(skip, c, carry):
            x, source_x = line(s, c)
            for yz in range(s.ny * s.half):
                y, zp = yz // s.half, yz % s.half
                cell = 2 * (x * s.ny * s.half + yz)
                for j in range(3):
                    inside = skip and 0 <= y + j - 1 < s.ny
                    source = left[(source_x * s.py + y + j) * s.half + zp]
                    for e in range(3):
                        if not (inside and inner_z(s, zp, e)):
                            pair_block(s, c, yz, cell, source_x - x, j, e, source, low, high, kernel)
                if yz > 0:
                    apply_line(s, c, yz - 1, gains, kernel, sums)
            apply_line(s, c, s.ny * s.half - 1, gains, kernel, sums)
            return carry

        lax.fori_loop(0, combos_x(s), functools.partial(along_x, True), 0, unroll=True)
        lax.fori_loop(combos_x(s), combos_x(s) + 2, functools.partial(along_x, False), 0, unroll=2)

        flow, weight = flow_of(s, sums, conduct_own[...], temp_own[...])
        flow_out[...] = flow
        occupied = own[3 * s.cells : 4 * s.cells, :] > 0.0
        top = jnp.max(jnp.where(occupied, weight, 0.0), axis=0, keepdims=True)
        top_out[...] = top
        faces.pack_x(flow_out, top, up, down)

    cells, padded = f32(s.cells, slots), f32(s.padded, slots)
    return pl.pallas_call(
        body,
        out_shape=(
            kernel_shape(s),
            cells,
            padded,
            padded,
            cells,
            cells,
            f32(1, slots),
            *faces.x_messages(),
        ),
        input_output_aliases={0: 0},
        scratch_shapes=[
            fields.halo_shape,
            pltpu.VMEM((s.columns * s.half, slots, 128), jnp.bfloat16),
            pltpu.VMEM((s.padded, 8, slots), jnp.float32),
            pltpu.VMEM((s.cells * 8, slots), jnp.float32),
            pltpu.VMEM((9, s.padded, slots), jnp.float32),
        ],
        compiler_params=pltpu.CompilerParams(vmem_limit_bytes=room),
        name="outer_and_first_flow",
    )


def next_kernel(s, room, last):
    slots = s.slots
    faces = Faces(s, 1)
    arrivals = len(faces.z_messages())

    def body(kernel, volume, scaled, conduct_own, *rest):
        if last:
            temp_own, flow1, *rest = rest
        own, top, x0, x1, y0, y1, *rest = rest
        z, rest = rest[:arrivals], rest[arrivals:]
        if last:
            out, temp, gains, sums, *rest = rest
        else:
            flow_out, top_out, up, down, temp, gains, sums = rest
        faces.lay_out(temp, own, x0, x1, y0, y1, z)
        most = faces.latest_top(top, z)
        source_rows(s, volume, scaled, temp, gains)

        sums[...] = jnp.zeros_like(sums)

        def along_x(c, carry):
            for yz in range(s.ny * s.half):
                apply_line(s, c, yz, gains, kernel, sums)
            return carry

        lax.fori_loop(0, combos_x(s) + 2, along_x, 0, unroll=3)
        flow, _ = flow_of(s, sums, conduct_own[...], own[...])
        if last and covered():
            rows, block, arrived = rest
            step = step_factor / jnp.max(most, axis=1, keepdims=True)
            rows[...] = polynomial(temp_own[...], step, flow1[...], own[...], flow)
            for x in range(s.nx):
                for y in range(s.ny):
                    start = (x * s.ny + y) * s.nz
                    block[x, y] = rows[start : start + s.nz, :]
            copy = pltpu.make_async_copy(block, out, arrived)
            copy.start()
            copy.wait()
        elif last:
            out[...] = flow
        else:
            flow_out[...] = flow
            top_out[...] = most
            faces.pack_x(flow_out, most, up, down)

    cells, shape = f32(s.cells, slots), (s.nx, s.ny, s.nz, slots)
    outs = (cells, f32(1, slots), *faces.x_messages())
    spaces = [pltpu.VMEM] * len(outs)
    scratch = [
        faces.halo_shape,
        pltpu.VMEM((s.padded, 8, slots), jnp.float32),
        pltpu.VMEM((s.cells * 8, slots), jnp.float32),
    ]
    if last and covered():
        outs, spaces = (f32(*shape),), [pl.ANY]
        scratch += [pltpu.VMEM((s.cells, slots), jnp.float32), pltpu.VMEM(shape, jnp.float32), pltpu.SemaphoreType.DMA]
    elif last:
        outs, spaces = (cells,), [pltpu.VMEM]
    return pl.pallas_call(
        body,
        out_shape=outs,
        out_specs=tuple(pl.BlockSpec(memory_space=space) for space in spaces),
        scratch_shapes=scratch,
        compiler_params=pltpu.CompilerParams(vmem_limit_bytes=room),
        name="last_flow" if last else "next_flow",
    )


def covered():
    return all(lax.axis_size(axis) <= 5 for axis in AXES)


def polynomial(start, step, flow1, flow2, flow3):
    return start + step * (flow1 + step * (0.5 * flow2 + step * (1.0 / 15.0) * flow3))


def local(relative_placements, mass_per_density, opening_heat_level, bin_fill_counts):
    nx, ny, nz, slots = opening_heat_level.shape
    s = Sizes(nx, ny, nz, slots)
    fields, faces = Faces(s, FIELDS), Faces(s, 1)
    arguments = (bin_fill_counts, relative_placements, mass_per_density, opening_heat_level)
    started = start_kernel(s)(*[pltpu.with_memory_space_constraint(a, pltpu.HBM) for a in arguments])
    made = []
    own_bytes = 4 * slots * rounded_up(FIELDS * s.cells)
    parts = (0, combos_x(s) // 7, 4 * combos_x(s) // 7, combos_x(s))

    def during(phase, after):
        begin, end = parts[phase], parts[phase + 1]
        if phase == 0:
            *outs, done = inner_kernel(s, ROOM - own_bytes - 4096, begin, end)(started[0], after)
            made.extend(outs)
        else:
            made[0], done = inner_kernel(s, ROOM, begin, end)(*made, after)
        return done

    own, _, *messages = fields.exchange(*started, during)
    kernel, low, high, _ = made
    kernel, flow1, volume, scaled, conduct_own, temp_own, top, up, down = outer_kernel(s, ROOM - own_bytes)(
        kernel, low, high, own, *messages
    )
    arrived = faces.exchange(flow1, top, up, down)
    flow2, top, up, down = next_kernel(s, ROOM, False)(kernel, volume, scaled, conduct_own, *arrived)
    arrived = faces.exchange(flow2, top, up, down)
    (final,) = next_kernel(s, ROOM, True)(kernel, volume, scaled, conduct_own, temp_own, flow1, *arrived)
    if not covered():
        top, flow3 = lax.optimization_barrier((arrived[1], final))
        step = step_factor / lax.pmax(jnp.max(top), AXES)
        final = polynomial(temp_own, step, flow1, flow2, flow3).reshape(nx, ny, nz, slots)
    return final


def solution(mesh):
    in_specs = (
        P(None, "gx", "gy", "gz", None),
        P("gx", "gy", "gz", None),
        P("gx", "gy", "gz", None),
        P("gx", "gy", "gz"),
    )
    out_specs = P("gx", "gy", "gz", None)
    return jax.shard_map(local, mesh=mesh, in_specs=in_specs, out_specs=out_specs, check_vma=False)
```

```python
import functools

import jax
import jax.numpy as jnp
from jax import lax
from jax.experimental import pallas as pl
from jax.experimental.pallas import tpu as pltpu
from jax.sharding import PartitionSpec as P

step_factor = 2.0
AXES = ("gx", "gy", "gz")
ROUNDER = 192.0
SHIFTS = (-1, 0, 1)
FIELDS = 5
ROOM = 8 << 20
SMALL = pltpu.CompilerParams(vmem_limit_bytes=2 << 20)


def route(axis, distance):
    size = lax.axis_size(axis)
    return [(i, (i + distance) % size) for i in range(size)]


def rounded_up(rows):
    return -(-rows // 8) * 8


def f32(*shape):
    return jax.ShapeDtypeStruct(shape, jnp.float32)


class Sizes:
    def __init__(self, nx, ny, nz, slots):
        self.nx, self.ny, self.nz, self.slots = nx, ny, nz, slots
        self.px, self.py, self.pz = nx + 2, ny + 2, nz + 2
        self.cells = nx * ny * nz
        self.padded = self.px * self.py * self.pz
        self.half = nz // 2
        self.pairs = nx * ny * self.half
        self.columns = self.px * self.py


class Faces:
    def __init__(self, s, fields):
        self.s, self.fields = s, fields
        self.x_rows = s.ny * s.nz
        self.y_rows = s.px * s.nz
        self.joined = lax.axis_size("gz") == 2
        self.z_rows = s.px * s.py
        self.z_faces = 2 if self.joined else 1
        self.halo_shape = pltpu.VMEM((fields * s.padded, s.slots), jnp.float32)

    def message(self, rows):
        return f32(rounded_up(self.fields * rows + 1), self.s.slots)

    def x_messages(self):
        return (self.message(self.x_rows),) * 2

    def y_messages(self):
        return (self.message(self.y_rows),) * 2

    def z_messages(self):
        return (self.message(self.z_faces * self.z_rows),) * (2 // self.z_faces)

    def row(self, f, x, y, z):
        return f * self.s.padded + (x * self.s.py + y) * self.s.pz + z

    def put_own(self, halo, own):
        s = self.s
        for f in range(self.fields):
            for x in range(s.nx):
                for y in range(s.ny):
                    at, start = self.row(f, x + 1, y + 1, 1), f * s.cells + (x * s.ny + y) * s.nz
                    halo[at : at + s.nz, :] = own[start : start + s.nz, :]

    def put_x(self, halo, before, after):
        s = self.s
        for f in range(self.fields):
            for side, x in ((before, 0), (after, s.nx + 1)):
                for y in range(s.ny):
                    at, start = self.row(f, x, y + 1, 1), f * self.x_rows + y * s.nz
                    halo[at : at + s.nz, :] = side[start : start + s.nz, :]

    def put_y(self, halo, before, after):
        s = self.s
        for f in range(self.fields):
            for side, y in ((before, 0), (after, s.ny + 1)):
                for x in range(s.px):
                    at, start = self.row(f, x, y, 1), f * self.y_rows + x * s.nz
                    halo[at : at + s.nz, :] = side[start : start + s.nz, :]

    def z_places(self, below, above):
        for f in range(self.fields):
            for k, z in ((0, below), (1, above)):
                m, base = (0, k * self.z_rows) if self.joined else (k, 0)
                for column in range(self.z_rows):
                    yield m, f * self.z_faces * self.z_rows + base + column, f, column, z

    def put_z(self, halo, sides):
        for m, start, f, column, z in self.z_places(0, self.s.nz + 1):
            at = f * self.s.padded + column * self.s.pz + z
            halo[at : at + 1, :] = sides[m][start : start + 1, :]

    def end(self, message, rows, top):
        n = self.fields * rows
        message[n : n + 1, :] = top

    def pack_x(self, own, top, up, down):
        s = self.s
        n = self.x_rows
        for f in range(self.fields):
            up[f * n : f * n + n, :] = own[f * s.cells + (s.nx - 1) * n : f * s.cells + s.nx * n, :]
            down[f * n : f * n + n, :] = own[f * s.cells : f * s.cells + n, :]
        for m in (up, down):
            self.end(m, n, top)

    def pack_y(self, halo, top, up, down):
        s = self.s
        for f in range(self.fields):
            for x in range(s.px):
                for m, y in ((up, s.ny), (down, 1)):
                    at, start = self.row(f, x, y, 1), f * self.y_rows + x * s.nz
                    m[start : start + s.nz, :] = halo[at : at + s.nz, :]
        for m in (up, down):
            self.end(m, self.y_rows, top)

    def pack_z(self, halo, top, messages):
        for m, start, f, column, z in self.z_places(self.s.nz, 1):
            at = f * self.s.padded + column * self.s.pz + z
            messages[m][start : start + 1, :] = halo[at : at + 1, :]
        for m in messages:
            self.end(m, self.z_faces * self.z_rows, top)

    def largest(self, top, rows, refs):
        n = self.fields * rows
        return jnp.maximum(top[...], jnp.maximum(refs[0][n : n + 1, :], refs[-1][n : n + 1, :]))

    def y_packer(self, waits):
        def body(own, top, before, after, *rest):
            up, down, top_out, halo = rest[waits:]
            self.put_own(halo, own)
            self.put_x(halo, before, after)
            most = self.largest(top, self.x_rows, (before, after))
            top_out[...] = most
            self.pack_y(halo, most, up, down)

        return pl.pallas_call(
            body,
            out_shape=(*self.y_messages(), f32(1, self.s.slots)),
            scratch_shapes=[self.halo_shape],
            compiler_params=SMALL,
            name="pack_y",
        )

    def z_packer(self, waits):
        count = len(self.z_messages())

        def body(own, top, x0, x1, y0, y1, *rest):
            rest = rest[waits:]
            messages, top_out, halo = rest[:count], rest[count], rest[-1]
            self.put_own(halo, own)
            self.put_x(halo, x0, x1)
            self.put_y(halo, y0, y1)
            most = self.largest(top, self.y_rows, (y0, y1))
            top_out[...] = most
            self.pack_z(halo, most, messages)

        return pl.pallas_call(
            body,
            out_shape=(*self.z_messages(), f32(1, self.s.slots)),
            scratch_shapes=[self.halo_shape],
            compiler_params=SMALL,
            name="pack_z",
        )

    def exchange(self, own, top, up, down, during=None):
        def beside(phase, top, *messages):
            done = None if during is None else during(phase, top, *messages)
            return () if done is None else (done,)

        x0 = lax.ppermute(up, "gx", route("gx", 1))
        x1 = lax.ppermute(down, "gx", route("gx", -1))
        waits = beside(0, top)
        up, down, top = self.y_packer(len(waits))(own, top, x0, x1, *waits)
        y0 = lax.ppermute(up, "gy", route("gy", 1))
        y1 = lax.ppermute(down, "gy", route("gy", -1))
        waits = beside(1, top)
        *messages, top = self.z_packer(len(waits))(own, top, x0, x1, y0, y1, *waits)
        z = [lax.ppermute(m, "gz", route("gz", d)) for m, d in zip(messages, (1, -1))]
        beside(2, top, own, x0, x1, y0, y1)
        return (own, top, x0, x1, y0, y1, *z)

    def lay_out(self, halo, own, x0, x1, y0, y1, z):
        self.put_own(halo, own)
        self.put_x(halo, x0, x1)
        self.put_y(halo, y0, y1)
        self.put_z(halo, z)

    def latest_top(self, top, z):
        return self.largest(top, self.z_faces * self.z_rows, z)


def rounded(x):
    return x.astype(jnp.bfloat16).astype(jnp.float32)


def split3(x):
    a = rounded(x)
    b = rounded(x - a)
    return a, b, x - a - b


def start_kernel(s):
    faces = Faces(s, FIELDS)

    def body(counts_in, placements_in, mass_in, temp_in, own, top_out, up, down,
             counts, placements, mass, temp, arrived):
        copies = [
            pltpu.make_async_copy(a, b, arrived.at[k])
            for k, (a, b) in enumerate(
                ((counts_in, counts), (placements_in, placements), (mass_in, mass), (temp_in, temp))
            )
        ]
        for copy in copies:
            copy.start()
        for copy in copies:
            copy.wait()
        slot = lax.broadcasted_iota(jnp.int32, (1, s.slots), 1)
        for x in range(s.nx):
            for y in range(s.ny):
                start = (x * s.ny + y) * s.nz
                for d in range(3):
                    own[d * s.cells + start : d * s.cells + start + s.nz, :] = placements[d, x, y]
                rows = [
                    jnp.where(slot < counts[x, y, z], mass[x, y, z : z + 1, :], 0.0) for z in range(s.nz)
                ]
                own[3 * s.cells + start : 3 * s.cells + start + s.nz, :] = jnp.concatenate(rows, axis=0)
                own[4 * s.cells + start : 4 * s.cells + start + s.nz, :] = temp[x, y]
        none = jnp.zeros((1, s.slots), jnp.float32)
        top_out[...] = none
        faces.pack_x(own, none, up, down)

    block = (s.nx, s.ny, s.nz, s.slots)
    return pl.pallas_call(
        body,
        in_specs=[pl.BlockSpec(memory_space=pltpu.HBM)] * 4,
        out_shape=(f32(FIELDS * s.cells, s.slots), f32(1, s.slots), *faces.x_messages()),
        scratch_shapes=[
            pltpu.SMEM(block[:3], jnp.int32),
            pltpu.VMEM((3, *block), jnp.float32),
            pltpu.VMEM(block, jnp.float32),
            pltpu.VMEM(block, jnp.float32),
            pltpu.SemaphoreType.DMA((4,)),
        ],
        compiler_params=SMALL,
        name="start",
    )


def source_rows(s, volume, scaled, temp, gains):
    row = lax.broadcasted_iota(jnp.int32, (8, s.slots), 0)
    use_c = (row % 4) < 2
    use_u = row < 4
    odd = (row % 2) == 1

    def one(cell, carry):
        def rows(ref):
            return jnp.broadcast_to(ref[pl.ds(cell, 1), :], (8, s.slots))

        full = jnp.where(use_c, rows(scaled), rows(volume)) * jnp.where(use_u, rows(temp), 1.0)
        top = rounded(full)
        gains[cell] = jnp.where(odd, full - top, top)
        return carry

    lax.fori_loop(0, s.padded, one, 0, unroll=6)


def gain_pair(gains, cell):
    return jnp.concatenate([gains[cell], gains[cell + 1]], axis=0).astype(jnp.bfloat16)


def add_sums(s, total, cell, sums):
    for k in range(2):
        rows = pl.ds(pl.multiple_of((cell + k) * 8, 8), 8)
        sums[rows, :] = sums[rows, :] + total[8 * k : 8 * k + 8, k * s.slots : (k + 1) * s.slots]


def flow_of(s, sums, conduct_own, temp_own):
    def of(r):
        return sums[pl.ds(r, s.cells, stride=8), :]

    weight = of(4) + of(5) + conduct_own * (of(6) + of(7))
    flow = of(0) + of(1) + conduct_own * (of(2) + of(3)) - temp_own * weight
    return flow, weight


def line(s, c):
    own = combos_x(s)
    x, side = (c + 1) // 3, c - own
    return (
        jnp.where(c < own, x, side * (s.nx - 1)),
        jnp.where(c < own, c - 2 * x + 1, side * (s.px - 1)),
    )


def apply_line(s, c, yz, gains, kernel, sums, chosen=None):
    x, source_x = line(s, c)
    y, zp = yz // s.half, yz % s.half
    blocks = [(j, e) for j in range(3) for e in range(3) if chosen is None or chosen(s, zp, e)]
    if not blocks:
        return
    parts = [gain_pair(gains, (source_x * s.py + y + j) * s.pz + 2 * zp + e) for j, e in blocks]
    if len(blocks) == 9:
        right = kernel[c, yz]
    else:
        right = jnp.concatenate(
            [kernel[c, yz, (j * 3 + e) * s.slots : (j * 3 + e + 1) * s.slots, :] for j, e in blocks], axis=0
        )
    total = jnp.dot(jnp.concatenate(parts, axis=1), right, preferred_element_type=jnp.float32)
    add_sums(s, total, 2 * (x * s.ny * s.half + yz), sums)


def kernel_shape(s):
    return jax.ShapeDtypeStruct((combos_x(s) + 2, s.ny * s.half, 9 * s.slots, 2 * s.slots), jnp.bfloat16)


def conductivity(temp):
    return temp * temp * jnp.sqrt(temp)


def rows_of(s, k, ref, cell):
    return jnp.broadcast_to(ref[k, pl.ds(cell, 1), :], (8, s.slots))


def on_grid(ref, d, count):
    return (ref[d * count : (d + 1) * count, :] - 0.5 + ROUNDER) - ROUNDER


def source_tables(s, ref, count, halves):
    square = 0.0
    for d in range(3):
        q = on_grid(ref, d, count)
        halves[2 * d] = rounded(q)
        halves[2 * d + 1] = q - rounded(q)
        square = square + q * q
    for d, part in enumerate(split3(square)):
        halves[6 + d] = part


def source_quads(s, halves, first_cell, present, left, at):
    row = lax.broadcasted_iota(jnp.int32, (8, s.slots), 0)
    zero8 = jnp.zeros((8, s.slots), jnp.float32)
    blocks = []
    for z in range(s.pz):
        if z not in present:
            blocks += [zero8] * 4
            continue
        cell = first_cell + present.index(z)
        for d in range(3):
            block = jnp.where(row % 2 == 0, rows_of(s, 2 * d, halves, cell), rows_of(s, 2 * d + 1, halves, cell))
            rest = jnp.where(row < 7, 1.0, rows_of(s, 6 + d, halves, cell))
            blocks.append(jnp.where(row < 4, block, rest))
        blocks.append(zero8)
    for zp in range(s.half):
        quad = jnp.concatenate(blocks[8 * zp : 8 * zp + 16], axis=0)
        left[at * s.half + zp] = quad.T.astype(jnp.bfloat16)


def target_tables(s, own, targets):
    for d in range(3):
        q = on_grid(own, d, s.cells)
        for k, shift in enumerate(SHIFTS):
            t = q - float(shift)
            h = rounded(t)
            for r, part in enumerate((-2.0 * h, -2.0 * (t - h), *split3(t * t))):
                targets[(d * 3 + k) * 5 + r] = part


def target_blocks(s, targets, cell, low, high):
    row = lax.broadcasted_iota(jnp.int32, (8, s.slots), 0)
    rows = []
    for d in range(3):
        for k in range(3):
            part = [rows_of(s, (d * 3 + k) * 5 + r, targets, cell) for r in range(5)]
            block = jnp.where(row == 5, part[3], jnp.where(row == 6, part[4], 1.0))
            block = jnp.where(row < 4, part[1], jnp.where(row == 4, part[2], block))
            rows.append(jnp.where(row < 2, part[0], block))
    for i in range(3):
        for j in range(3):
            low[cell * 9 + i * 3 + j] = jnp.concatenate([rows[i], rows[3 + j]], 0).astype(jnp.bfloat16)
    for e in range(3):
        high[cell * 3 + e] = jnp.concatenate([rows[6 + e], jnp.zeros_like(rows[0])], 0).astype(jnp.bfloat16)


def pair_block(s, c, yz, cell, i, j, e, source, low, high, kernel):
    nothing = jnp.zeros((16, s.slots), jnp.bfloat16)
    lanes = []
    for k in range(2):
        parts = [nothing] * 8
        parts[2 * (e + k)] = low[(cell + k) * 9 + i * 3 + j]
        parts[2 * (e + k) + 1] = high[(cell + k) * 3 + e]
        lanes.append(jnp.concatenate(parts, axis=0))
    right = jnp.concatenate(lanes, axis=1)
    dist = jnp.dot(source, right, preferred_element_type=jnp.float32)
    gap = 1.0 - dist * lax.rsqrt(jnp.maximum(dist, 2.5e-7))
    value = jnp.maximum((gap * gap * gap).astype(jnp.bfloat16), jnp.bfloat16(0.0))
    kernel[c, yz, (j * 3 + e) * s.slots : (j * 3 + e + 1) * s.slots, :] = value


def inner_z(s, zp, e):
    return 0 <= 2 * zp + e - 1 and 2 * zp + e < s.nz


def outer_z(s, zp, e):
    return not inner_z(s, zp, e)


def combos_x(s):
    return 3 * s.nx - 2


def inner_kernel(s, room, begin, end):
    slots = s.slots
    opening = begin == 0

    def blocks(left, low, high, kernel):
        def along_x(c, carry):
            x, source_x = line(s, c)
            for yz in range(s.ny * s.half):
                y, zp = yz // s.half, yz % s.half
                cell = 2 * (x * s.ny * s.half + yz)
                for j in range(3):
                    if not 0 <= y + j - 1 < s.ny:
                        continue
                    source = left[((source_x - 1) * s.ny + y + j - 1) * s.half + zp]
                    for e in range(3):
                        if inner_z(s, zp, e):
                            pair_block(s, c, yz, cell, source_x - x, j, e, source, low, high, kernel)
            return carry

        lax.fori_loop(begin, end, along_x, 0, unroll=True)

    def first(own, after, kernel, low, high, left, done, halves, targets):
        done[...] = after[...]
        source_tables(s, own, s.cells, halves)
        target_tables(s, own, targets)

        def prepare(column, carry):
            source_quads(s, halves, column * s.nz, list(range(1, s.nz + 1)), left, column)
            for z in range(s.nz):
                target_blocks(s, targets, column * s.nz + z, low, high)
            return carry

        lax.fori_loop(0, s.nx * s.ny, prepare, 0)
        blocks(left, low, high, kernel)

    def second(kernel_in, low, high, left, after, kernel, done):
        done[...] = after[...]
        blocks(left, low, high, kernel)

    kernel = kernel_shape(s)
    if opening:
        return pl.pallas_call(
            first,
            out_shape=(
                kernel,
                jax.ShapeDtypeStruct((s.cells * 9, 16, slots), jnp.bfloat16),
                jax.ShapeDtypeStruct((s.cells * 3, 16, slots), jnp.bfloat16),
                jax.ShapeDtypeStruct((s.pairs, slots, 128), jnp.bfloat16),
                f32(1, slots),
            ),
            scratch_shapes=[
                pltpu.VMEM((9, s.cells, slots), jnp.float32),
                pltpu.VMEM((45, s.cells, slots), jnp.float32),
            ],
            compiler_params=pltpu.CompilerParams(vmem_limit_bytes=room),
            name="inner_first",
        )
    return pl.pallas_call(
        second,
        out_shape=(kernel, f32(1, slots)),
        input_output_aliases={0: 0},
        compiler_params=pltpu.CompilerParams(vmem_limit_bytes=room),
        name="inner_second",
    )


def outer_kernel(s, room):
    slots = s.slots
    fields = Faces(s, FIELDS)
    faces = Faces(s, 1)
    arrivals = len(fields.z_messages())

    def body(kernel_in, low, high, own, x0, x1, y0, y1, *rest):
        z, rest = rest[:arrivals], rest[arrivals:]
        (kernel, flow_out, volume_out, scaled_out, conduct_own, temp_own, top_out, up, down,
         halo, left, gains, sums, halves) = rest
        fields.lay_out(halo, own, x0, x1, y0, y1, z)
        temp = halo.at[pl.ds(4 * s.padded, s.padded)]
        volume_out[...] = halo[3 * s.padded : 4 * s.padded, :]
        scaled_out[...] = volume_out[...] * conductivity(temp[...])
        temp_own[...] = own[4 * s.cells : 5 * s.cells, :]
        conduct_own[...] = conductivity(temp_own[...])
        source_rows(s, volume_out, scaled_out, temp, gains)
        source_tables(s, halo, s.padded, halves)

        def features(column, carry):
            source_quads(s, halves, column * s.pz, list(range(s.pz)), left, column)
            return carry

        lax.fori_loop(0, s.columns, features, 0, unroll=5)

        sums[...] = jnp.zeros_like(sums)

        def along_x(skip, c, carry):
            x, source_x = line(s, c)
            for yz in range(s.ny * s.half):
                y, zp = yz // s.half, yz % s.half
                cell = 2 * (x * s.ny * s.half + yz)
                for j in range(3):
                    inside = skip and 0 <= y + j - 1 < s.ny
                    source = left[(source_x * s.py + y + j) * s.half + zp]
                    for e in range(3):
                        if not (inside and inner_z(s, zp, e)):
                            pair_block(s, c, yz, cell, source_x - x, j, e, source, low, high, kernel)
                if yz > 0:
                    apply_line(s, c, yz - 1, gains, kernel, sums)
            apply_line(s, c, s.ny * s.half - 1, gains, kernel, sums)
            return carry

        lax.fori_loop(0, combos_x(s), functools.partial(along_x, True), 0, unroll=True)
        lax.fori_loop(combos_x(s), combos_x(s) + 2, functools.partial(along_x, False), 0, unroll=2)

        flow, weight = flow_of(s, sums, conduct_own[...], temp_own[...])
        flow_out[...] = flow
        occupied = own[3 * s.cells : 4 * s.cells, :] > 0.0
        top = jnp.max(jnp.where(occupied, weight, 0.0), axis=0, keepdims=True)
        top_out[...] = top
        faces.pack_x(flow_out, top, up, down)

    cells, padded = f32(s.cells, slots), f32(s.padded, slots)
    return pl.pallas_call(
        body,
        out_shape=(
            kernel_shape(s),
            cells,
            padded,
            padded,
            cells,
            cells,
            f32(1, slots),
            *faces.x_messages(),
        ),
        input_output_aliases={0: 0},
        scratch_shapes=[
            fields.halo_shape,
            pltpu.VMEM((s.columns * s.half, slots, 128), jnp.bfloat16),
            pltpu.VMEM((s.padded, 8, slots), jnp.float32),
            pltpu.VMEM((s.cells * 8, slots), jnp.float32),
            pltpu.VMEM((9, s.padded, slots), jnp.float32),
        ],
        compiler_params=pltpu.CompilerParams(vmem_limit_bytes=room),
        name="outer_and_first_flow",
    )


def part_kernel(s, room):
    slots = s.slots
    faces = Faces(s, 1)

    def body(kernel, volume, scaled, after, own, x0, x1, y0, y1, sums, temp, gains):
        faces.put_own(temp, own)
        faces.put_x(temp, x0, x1)
        faces.put_y(temp, y0, y1)
        none = jnp.zeros((1, slots), jnp.float32)
        for column in range(s.columns):
            for z in (0, s.pz - 1):
                temp[column * s.pz + z : column * s.pz + z + 1, :] = none
        source_rows(s, volume, scaled, temp, gains)
        sums[...] = jnp.zeros_like(sums)

        def along_x(c, carry):
            for yz in range(s.ny * s.half):
                apply_line(s, c, yz, gains, kernel, sums, inner_z)
            return carry

        lax.fori_loop(0, combos_x(s) + 2, along_x, 0, unroll=3)

    return pl.pallas_call(
        body,
        out_shape=f32(s.cells * 8, slots),
        scratch_shapes=[faces.halo_shape, pltpu.VMEM((s.padded, 8, slots), jnp.float32)],
        compiler_params=pltpu.CompilerParams(vmem_limit_bytes=room),
        name="part_flow",
    )


def next_kernel(s, room, last):
    slots = s.slots
    faces = Faces(s, 1)
    arrivals = len(faces.z_messages())

    def body(kernel, volume, scaled, conduct_own, part, *rest):
        if last:
            temp_own, flow1, *rest = rest
        own, top, x0, x1, y0, y1, *rest = rest
        z, rest = rest[:arrivals], rest[arrivals:]
        if last:
            out, temp, gains, sums, *rest = rest
        else:
            flow_out, top_out, up, down, temp, gains, sums = rest
        faces.lay_out(temp, own, x0, x1, y0, y1, z)
        most = faces.latest_top(top, z)
        source_rows(s, volume, scaled, temp, gains)

        sums[...] = part[...]

        def along_x(c, carry):
            for yz in range(s.ny * s.half):
                apply_line(s, c, yz, gains, kernel, sums, outer_z)
            return carry

        lax.fori_loop(0, combos_x(s) + 2, along_x, 0, unroll=3)
        flow, _ = flow_of(s, sums, conduct_own[...], own[...])
        if last and covered():
            rows, block, arrived = rest
            step = step_factor / jnp.max(most, axis=1, keepdims=True)
            rows[...] = polynomial(temp_own[...], step, flow1[...], own[...], flow)
            for x in range(s.nx):
                for y in range(s.ny):
                    start = (x * s.ny + y) * s.nz
                    block[x, y] = rows[start : start + s.nz, :]
            copy = pltpu.make_async_copy(block, out, arrived)
            copy.start()
            copy.wait()
        elif last:
            out[...] = flow
        else:
            flow_out[...] = flow
            top_out[...] = most
            faces.pack_x(flow_out, most, up, down)

    cells, shape = f32(s.cells, slots), (s.nx, s.ny, s.nz, slots)
    outs = (cells, f32(1, slots), *faces.x_messages())
    spaces = [pltpu.VMEM] * len(outs)
    scratch = [
        faces.halo_shape,
        pltpu.VMEM((s.padded, 8, slots), jnp.float32),
        pltpu.VMEM((s.cells * 8, slots), jnp.float32),
    ]
    if last and covered():
        outs, spaces = (f32(*shape),), [pl.ANY]
        scratch += [pltpu.VMEM((s.cells, slots), jnp.float32), pltpu.VMEM(shape, jnp.float32), pltpu.SemaphoreType.DMA]
    elif last:
        outs, spaces = (cells,), [pltpu.VMEM]
    return pl.pallas_call(
        body,
        out_shape=outs,
        out_specs=tuple(pl.BlockSpec(memory_space=space) for space in spaces),
        scratch_shapes=scratch,
        compiler_params=pltpu.CompilerParams(vmem_limit_bytes=room),
        name="last_flow" if last else "next_flow",
    )


def covered():
    return all(lax.axis_size(axis) <= 5 for axis in AXES)


def polynomial(start, step, flow1, flow2, flow3):
    return start + step * (flow1 + step * (0.5 * flow2 + step * (1.0 / 15.0) * flow3))


def local(relative_placements, mass_per_density, opening_heat_level, bin_fill_counts):
    nx, ny, nz, slots = opening_heat_level.shape
    s = Sizes(nx, ny, nz, slots)
    fields, faces = Faces(s, FIELDS), Faces(s, 1)
    arguments = (bin_fill_counts, relative_placements, mass_per_density, opening_heat_level)
    started = start_kernel(s)(*[pltpu.with_memory_space_constraint(a, pltpu.HBM) for a in arguments])
    made = []
    own_bytes = 4 * slots * rounded_up(FIELDS * s.cells)
    parts = (0, combos_x(s) // 7, 4 * combos_x(s) // 7, combos_x(s))

    def during(phase, after, *_):
        begin, end = parts[phase], parts[phase + 1]
        if phase == 0:
            *outs, done = inner_kernel(s, ROOM - own_bytes - 4096, begin, end)(started[0], after)
            made.extend(outs)
        else:
            made[0], done = inner_kernel(s, ROOM, begin, end)(*made, after)
        return done

    own, _, *messages = fields.exchange(*started, during)
    kernel, low, high, _ = made
    kernel, flow1, volume, scaled, conduct_own, temp_own, top, up, down = outer_kernel(s, ROOM - own_bytes)(
        kernel, low, high, own, *messages
    )
    sums = []

    def apply_part(phase, after, *messages):
        if phase == 2:
            sums.append(part_kernel(s, ROOM)(kernel, volume, scaled, after, *messages))

    arrived = faces.exchange(flow1, top, up, down, apply_part)
    flow2, top, up, down = next_kernel(s, ROOM, False)(kernel, volume, scaled, conduct_own, sums[0], *arrived)
    arrived = faces.exchange(flow2, top, up, down, apply_part)
    (final,) = next_kernel(s, ROOM, True)(
        kernel, volume, scaled, conduct_own, sums[1], temp_own, flow1, *arrived
    )
    if not covered():
        top, flow3 = lax.optimization_barrier((arrived[1], final))
        step = step_factor / lax.pmax(jnp.max(top), AXES)
        final = polynomial(temp_own, step, flow1, flow2, flow3).reshape(nx, ny, nz, slots)
    return final


def solution(mesh):
    in_specs = (
        P(None, "gx", "gy", "gz", None),
        P("gx", "gy", "gz", None),
        P("gx", "gy", "gz", None),
        P("gx", "gy", "gz"),
    )
    out_specs = P("gx", "gy", "gz", None)
    return jax.shard_map(local, mesh=mesh, in_specs=in_specs, out_specs=out_specs, check_vma=False)
```

```python
import functools

import jax
import jax.numpy as jnp
from jax import lax
from jax.experimental import pallas as pl
from jax.experimental.pallas import tpu as pltpu
from jax.sharding import PartitionSpec as P

step_factor = 2.0
AXES = ("gx", "gy", "gz")
ROUNDER = 192.0
SHIFTS = (-1, 0, 1)
FIELDS = 5
ROOM = 8 << 20
SMALL = pltpu.CompilerParams(vmem_limit_bytes=2 << 20)


def route(axis, distance):
    size = lax.axis_size(axis)
    return [(i, (i + distance) % size) for i in range(size)]


def rounded_up(rows):
    return -(-rows // 8) * 8


def f32(*shape):
    return jax.ShapeDtypeStruct(shape, jnp.float32)


class Sizes:
    def __init__(self, nx, ny, nz, slots):
        self.nx, self.ny, self.nz, self.slots = nx, ny, nz, slots
        self.px, self.py, self.pz = nx + 2, ny + 2, nz + 2
        self.cells = nx * ny * nz
        self.padded = self.px * self.py * self.pz
        self.half = nz // 2
        self.pairs = nx * ny * self.half
        self.columns = self.px * self.py


class Faces:
    def __init__(self, s, fields):
        self.s, self.fields = s, fields
        self.x_rows = s.ny * s.nz
        self.y_rows = s.px * s.nz
        self.joined = lax.axis_size("gz") == 2
        self.z_rows = s.px * s.py
        self.z_faces = 2 if self.joined else 1
        self.halo_shape = pltpu.VMEM((fields * s.padded, s.slots), jnp.float32)

    def message(self, rows):
        return f32(rounded_up(self.fields * rows + 1), self.s.slots)

    def x_messages(self):
        return (self.message(self.x_rows),) * 2

    def y_messages(self):
        return (self.message(self.y_rows),) * 2

    def z_messages(self):
        return (self.message(self.z_faces * self.z_rows),) * (2 // self.z_faces)

    def row(self, f, x, y, z):
        return f * self.s.padded + (x * self.s.py + y) * self.s.pz + z

    def put_own(self, halo, own):
        s = self.s
        for f in range(self.fields):
            for x in range(s.nx):
                for y in range(s.ny):
                    at, start = self.row(f, x + 1, y + 1, 1), f * s.cells + (x * s.ny + y) * s.nz
                    halo[at : at + s.nz, :] = own[start : start + s.nz, :]

    def put_x(self, halo, before, after):
        s = self.s
        for f in range(self.fields):
            for side, x in ((before, 0), (after, s.nx + 1)):
                for y in range(s.ny):
                    at, start = self.row(f, x, y + 1, 1), f * self.x_rows + y * s.nz
                    halo[at : at + s.nz, :] = side[start : start + s.nz, :]

    def put_y(self, halo, before, after):
        s = self.s
        for f in range(self.fields):
            for side, y in ((before, 0), (after, s.ny + 1)):
                for x in range(s.px):
                    at, start = self.row(f, x, y, 1), f * self.y_rows + x * s.nz
                    halo[at : at + s.nz, :] = side[start : start + s.nz, :]

    def z_places(self, below, above):
        for f in range(self.fields):
            for k, z in ((0, below), (1, above)):
                m, base = (0, k * self.z_rows) if self.joined else (k, 0)
                for column in range(self.z_rows):
                    yield m, f * self.z_faces * self.z_rows + base + column, f, column, z

    def put_z(self, halo, sides):
        for m, start, f, column, z in self.z_places(0, self.s.nz + 1):
            at = f * self.s.padded + column * self.s.pz + z
            halo[at : at + 1, :] = sides[m][start : start + 1, :]

    def end(self, message, rows, top):
        n = self.fields * rows
        message[n : n + 1, :] = top

    def pack_x(self, own, top, up, down):
        s = self.s
        n = self.x_rows
        for f in range(self.fields):
            up[f * n : f * n + n, :] = own[f * s.cells + (s.nx - 1) * n : f * s.cells + s.nx * n, :]
            down[f * n : f * n + n, :] = own[f * s.cells : f * s.cells + n, :]
        for m in (up, down):
            self.end(m, n, top)

    def pack_y(self, halo, top, up, down):
        s = self.s
        for f in range(self.fields):
            for x in range(s.px):
                for m, y in ((up, s.ny), (down, 1)):
                    at, start = self.row(f, x, y, 1), f * self.y_rows + x * s.nz
                    m[start : start + s.nz, :] = halo[at : at + s.nz, :]
        for m in (up, down):
            self.end(m, self.y_rows, top)

    def pack_z(self, halo, top, messages):
        for m, start, f, column, z in self.z_places(self.s.nz, 1):
            at = f * self.s.padded + column * self.s.pz + z
            messages[m][start : start + 1, :] = halo[at : at + 1, :]
        for m in messages:
            self.end(m, self.z_faces * self.z_rows, top)

    def largest(self, top, rows, refs):
        n = self.fields * rows
        return jnp.maximum(top[...], jnp.maximum(refs[0][n : n + 1, :], refs[-1][n : n + 1, :]))

    def y_packer(self, waits):
        def body(own, top, before, after, *rest):
            up, down, top_out, halo = rest[waits:]
            self.put_own(halo, own)
            self.put_x(halo, before, after)
            most = self.largest(top, self.x_rows, (before, after))
            top_out[...] = most
            self.pack_y(halo, most, up, down)

        return pl.pallas_call(
            body,
            out_shape=(*self.y_messages(), f32(1, self.s.slots)),
            scratch_shapes=[self.halo_shape],
            compiler_params=SMALL,
            name="pack_y",
        )

    def z_packer(self, waits):
        count = len(self.z_messages())

        def body(own, top, x0, x1, y0, y1, *rest):
            rest = rest[waits:]
            messages, top_out, halo = rest[:count], rest[count], rest[-1]
            self.put_own(halo, own)
            self.put_x(halo, x0, x1)
            self.put_y(halo, y0, y1)
            most = self.largest(top, self.y_rows, (y0, y1))
            top_out[...] = most
            self.pack_z(halo, most, messages)

        return pl.pallas_call(
            body,
            out_shape=(*self.z_messages(), f32(1, self.s.slots)),
            scratch_shapes=[self.halo_shape],
            compiler_params=SMALL,
            name="pack_z",
        )

    def exchange(self, own, top, up, down, during=None):
        def beside(phase, top, *messages):
            done = None if during is None else during(phase, top, *messages)
            return () if done is None else (done,)

        x0 = lax.ppermute(up, "gx", route("gx", 1))
        x1 = lax.ppermute(down, "gx", route("gx", -1))
        waits = beside(0, top)
        up, down, top = self.y_packer(len(waits))(own, top, x0, x1, *waits)
        y0 = lax.ppermute(up, "gy", route("gy", 1))
        y1 = lax.ppermute(down, "gy", route("gy", -1))
        waits = beside(1, top)
        *messages, top = self.z_packer(len(waits))(own, top, x0, x1, y0, y1, *waits)
        z = [lax.ppermute(m, "gz", route("gz", d)) for m, d in zip(messages, (1, -1))]
        beside(2, top, own, x0, x1, y0, y1)
        return (own, top, x0, x1, y0, y1, *z)

    def lay_out(self, halo, own, x0, x1, y0, y1, z):
        self.put_own(halo, own)
        self.put_x(halo, x0, x1)
        self.put_y(halo, y0, y1)
        self.put_z(halo, z)

    def latest_top(self, top, z):
        return self.largest(top, self.z_faces * self.z_rows, z)


def rounded(x):
    return x.astype(jnp.bfloat16).astype(jnp.float32)


def split3(x):
    a = rounded(x)
    b = rounded(x - a)
    return a, b, x - a - b


def start_kernel(s):
    faces = Faces(s, FIELDS)

    def body(counts_in, placements_in, mass_in, temp_in, own, top_out, up, down,
             counts, placements, mass, temp, arrived):
        copies = [
            pltpu.make_async_copy(a, b, arrived.at[k])
            for k, (a, b) in enumerate(
                ((counts_in, counts), (placements_in, placements), (mass_in, mass), (temp_in, temp))
            )
        ]
        for copy in copies:
            copy.start()
        for copy in copies:
            copy.wait()
        slot = lax.broadcasted_iota(jnp.int32, (1, s.slots), 1)
        for x in range(s.nx):
            for y in range(s.ny):
                start = (x * s.ny + y) * s.nz
                for d in range(3):
                    own[d * s.cells + start : d * s.cells + start + s.nz, :] = placements[d, x, y]
                rows = [
                    jnp.where(slot < counts[x, y, z], mass[x, y, z : z + 1, :], 0.0) for z in range(s.nz)
                ]
                own[3 * s.cells + start : 3 * s.cells + start + s.nz, :] = jnp.concatenate(rows, axis=0)
                own[4 * s.cells + start : 4 * s.cells + start + s.nz, :] = temp[x, y]
        none = jnp.zeros((1, s.slots), jnp.float32)
        top_out[...] = none
        faces.pack_x(own, none, up, down)

    block = (s.nx, s.ny, s.nz, s.slots)
    return pl.pallas_call(
        body,
        in_specs=[pl.BlockSpec(memory_space=pltpu.HBM)] * 4,
        out_shape=(f32(FIELDS * s.cells, s.slots), f32(1, s.slots), *faces.x_messages()),
        scratch_shapes=[
            pltpu.SMEM(block[:3], jnp.int32),
            pltpu.VMEM((3, *block), jnp.float32),
            pltpu.VMEM(block, jnp.float32),
            pltpu.VMEM(block, jnp.float32),
            pltpu.SemaphoreType.DMA((4,)),
        ],
        compiler_params=SMALL,
        name="start",
    )


def source_rows(s, volume, scaled, temp, gains):
    row = lax.broadcasted_iota(jnp.int32, (8, s.slots), 0)
    use_c = (row % 4) < 2
    use_u = row < 4
    odd = (row % 2) == 1

    def one(cell, carry):
        def rows(ref):
            return jnp.broadcast_to(ref[pl.ds(cell, 1), :], (8, s.slots))

        full = jnp.where(use_c, rows(scaled), rows(volume)) * jnp.where(use_u, rows(temp), 1.0)
        top = rounded(full)
        gains[cell] = jnp.where(odd, full - top, top)
        return carry

    lax.fori_loop(0, s.padded, one, 0, unroll=6)


def gain_pair(gains, cell):
    return jnp.concatenate([gains[cell], gains[cell + 1]], axis=0).astype(jnp.bfloat16)


def add_sums(s, total, cell, sums):
    for k in range(2):
        rows = pl.ds(pl.multiple_of((cell + k) * 8, 8), 8)
        sums[rows, :] = sums[rows, :] + total[8 * k : 8 * k + 8, k * s.slots : (k + 1) * s.slots]


def flow_of(s, sums, conduct_own, temp_own):
    def of(r):
        return sums[pl.ds(r, s.cells, stride=8), :]

    weight = of(4) + of(5) + conduct_own * (of(6) + of(7))
    flow = of(0) + of(1) + conduct_own * (of(2) + of(3)) - temp_own * weight
    return flow, weight


def line(s, c):
    own = combos_x(s)
    x, side = (c + 1) // 3, c - own
    return (
        jnp.where(c < own, x, side * (s.nx - 1)),
        jnp.where(c < own, c - 2 * x + 1, side * (s.px - 1)),
    )


def apply_line(s, c, yz, gains, kernel, sums, chosen=None):
    x, source_x = line(s, c)
    y, zp = yz // s.half, yz % s.half
    blocks = [(j, e) for j in range(3) for e in range(3) if chosen is None or chosen(s, zp, e)]
    if not blocks:
        return
    parts = [gain_pair(gains, (source_x * s.py + y + j) * s.pz + 2 * zp + e) for j, e in blocks]
    if len(blocks) == 9:
        right = kernel[c, yz]
    else:
        right = jnp.concatenate(
            [kernel[c, yz, (j * 3 + e) * s.slots : (j * 3 + e + 1) * s.slots, :] for j, e in blocks], axis=0
        )
    total = jnp.dot(jnp.concatenate(parts, axis=1), right, preferred_element_type=jnp.float32)
    add_sums(s, total, 2 * (x * s.ny * s.half + yz), sums)


def kernel_shape(s):
    return jax.ShapeDtypeStruct((combos_x(s) + 2, s.ny * s.half, 9 * s.slots, 2 * s.slots), jnp.bfloat16)


def conductivity(temp):
    return temp * temp * jnp.sqrt(temp)


def rows_of(s, k, ref, cell):
    return jnp.broadcast_to(ref[k, pl.ds(cell, 1), :], (8, s.slots))


def on_grid(ref, d, count):
    return (ref[d * count : (d + 1) * count, :] - 0.5 + ROUNDER) - ROUNDER


def source_tables(s, ref, count, halves):
    square = 0.0
    for d in range(3):
        q = on_grid(ref, d, count)
        halves[2 * d] = rounded(q)
        halves[2 * d + 1] = q - rounded(q)
        square = square + q * q
    for d, part in enumerate(split3(square)):
        halves[6 + d] = part


def source_quads(s, halves, first_cell, present, left, at):
    row = lax.broadcasted_iota(jnp.int32, (8, s.slots), 0)
    zero8 = jnp.zeros((8, s.slots), jnp.float32)
    blocks = []
    for z in range(s.pz):
        if z not in present:
            blocks += [zero8] * 4
            continue
        cell = first_cell + present.index(z)
        for d in range(3):
            block = jnp.where(row % 2 == 0, rows_of(s, 2 * d, halves, cell), rows_of(s, 2 * d + 1, halves, cell))
            rest = jnp.where(row < 7, 1.0, rows_of(s, 6 + d, halves, cell))
            blocks.append(jnp.where(row < 4, block, rest))
        blocks.append(zero8)
    for zp in range(s.half):
        quad = jnp.concatenate(blocks[8 * zp : 8 * zp + 16], axis=0)
        left[at * s.half + zp] = quad.T.astype(jnp.bfloat16)


def target_tables(s, own, targets):
    for d in range(3):
        q = on_grid(own, d, s.cells)
        for k, shift in enumerate(SHIFTS):
            t = q - float(shift)
            h = rounded(t)
            for r, part in enumerate((-2.0 * h, -2.0 * (t - h), *split3(t * t))):
                targets[(d * 3 + k) * 5 + r] = part


def target_blocks(s, targets, cell, low, high):
    row = lax.broadcasted_iota(jnp.int32, (8, s.slots), 0)
    rows = []
    for d in range(3):
        for k in range(3):
            part = [rows_of(s, (d * 3 + k) * 5 + r, targets, cell) for r in range(5)]
            block = jnp.where(row == 5, part[3], jnp.where(row == 6, part[4], 1.0))
            block = jnp.where(row < 4, part[1], jnp.where(row == 4, part[2], block))
            rows.append(jnp.where(row < 2, part[0], block))
    for i in range(3):
        for j in range(3):
            low[cell * 9 + i * 3 + j] = jnp.concatenate([rows[i], rows[3 + j]], 0).astype(jnp.bfloat16)
    for e in range(3):
        high[cell * 3 + e] = jnp.concatenate([rows[6 + e], jnp.zeros_like(rows[0])], 0).astype(jnp.bfloat16)


def pair_block(s, c, yz, cell, i, j, e, source, low, high, kernel):
    nothing = jnp.zeros((16, s.slots), jnp.bfloat16)
    lanes = []
    for k in range(2):
        parts = [nothing] * 8
        parts[2 * (e + k)] = low[(cell + k) * 9 + i * 3 + j]
        parts[2 * (e + k) + 1] = high[(cell + k) * 3 + e]
        lanes.append(jnp.concatenate(parts, axis=0))
    right = jnp.concatenate(lanes, axis=1)
    dist = jnp.dot(source, right, preferred_element_type=jnp.float32)
    gap = 1.0 - dist * lax.rsqrt(jnp.maximum(dist, 2.5e-7))
    value = jnp.maximum((gap * gap * gap).astype(jnp.bfloat16), jnp.bfloat16(0.0))
    kernel[c, yz, (j * 3 + e) * s.slots : (j * 3 + e + 1) * s.slots, :] = value


def inner_z(s, zp, e):
    return 0 <= 2 * zp + e - 1 and 2 * zp + e < s.nz


def outer_z(s, zp, e):
    return not inner_z(s, zp, e)


def combos_x(s):
    return 3 * s.nx - 2


def inner_kernel(s, room, begin, end):
    slots = s.slots
    opening = begin == 0

    def blocks(left, low, high, kernel):
        def along_x(c, carry):
            x, source_x = line(s, c)
            for yz in range(s.ny * s.half):
                y, zp = yz // s.half, yz % s.half
                cell = 2 * (x * s.ny * s.half + yz)
                for j in range(3):
                    if not 0 <= y + j - 1 < s.ny:
                        continue
                    source = left[((source_x - 1) * s.ny + y + j - 1) * s.half + zp]
                    for e in range(3):
                        if inner_z(s, zp, e):
                            pair_block(s, c, yz, cell, source_x - x, j, e, source, low, high, kernel)
            return carry

        lax.fori_loop(begin, end, along_x, 0, unroll=True)

    def first(own, after, kernel, low, high, left, done, halves, targets):
        done[...] = after[...]
        source_tables(s, own, s.cells, halves)
        target_tables(s, own, targets)

        def prepare(column, carry):
            source_quads(s, halves, column * s.nz, list(range(1, s.nz + 1)), left, column)
            for z in range(s.nz):
                target_blocks(s, targets, column * s.nz + z, low, high)
            return carry

        lax.fori_loop(0, s.nx * s.ny, prepare, 0)
        blocks(left, low, high, kernel)

    def second(kernel_in, low, high, left, after, kernel, done):
        done[...] = after[...]
        blocks(left, low, high, kernel)

    kernel = kernel_shape(s)
    if opening:
        return pl.pallas_call(
            first,
            out_shape=(
                kernel,
                jax.ShapeDtypeStruct((s.cells * 9, 16, slots), jnp.bfloat16),
                jax.ShapeDtypeStruct((s.cells * 3, 16, slots), jnp.bfloat16),
                jax.ShapeDtypeStruct((s.pairs, slots, 128), jnp.bfloat16),
                f32(1, slots),
            ),
            scratch_shapes=[
                pltpu.VMEM((9, s.cells, slots), jnp.float32),
                pltpu.VMEM((45, s.cells, slots), jnp.float32),
            ],
            compiler_params=pltpu.CompilerParams(vmem_limit_bytes=room),
            name="inner_first",
        )
    return pl.pallas_call(
        second,
        out_shape=(kernel, f32(1, slots)),
        input_output_aliases={0: 0},
        compiler_params=pltpu.CompilerParams(vmem_limit_bytes=room),
        name="inner_second",
    )


def outer_kernel(s, room):
    slots = s.slots
    fields = Faces(s, FIELDS)
    faces = Faces(s, 1)
    arrivals = len(fields.z_messages())

    def body(kernel_in, low, high, own, x0, x1, y0, y1, *rest):
        z, rest = rest[:arrivals], rest[arrivals:]
        (kernel, flow_out, volume_out, scaled_out, conduct_own, temp_own, top_out, up, down,
         halo, left, gains, sums, halves) = rest
        fields.lay_out(halo, own, x0, x1, y0, y1, z)
        temp = halo.at[pl.ds(4 * s.padded, s.padded)]
        volume_out[...] = halo[3 * s.padded : 4 * s.padded, :]
        scaled_out[...] = volume_out[...] * conductivity(temp[...])
        temp_own[...] = own[4 * s.cells : 5 * s.cells, :]
        conduct_own[...] = conductivity(temp_own[...])
        source_rows(s, volume_out, scaled_out, temp, gains)
        source_tables(s, halo, s.padded, halves)

        def features(column, carry):
            source_quads(s, halves, column * s.pz, list(range(s.pz)), left, column)
            return carry

        lax.fori_loop(0, s.columns, features, 0, unroll=5)

        sums[...] = jnp.zeros_like(sums)

        def along_x(skip, c, carry):
            x, source_x = line(s, c)
            for yz in range(s.ny * s.half):
                y, zp = yz // s.half, yz % s.half
                cell = 2 * (x * s.ny * s.half + yz)
                for j in range(3):
                    inside = skip and 0 <= y + j - 1 < s.ny
                    source = left[(source_x * s.py + y + j) * s.half + zp]
                    for e in range(3):
                        if not (inside and inner_z(s, zp, e)):
                            pair_block(s, c, yz, cell, source_x - x, j, e, source, low, high, kernel)
                if yz > 0:
                    apply_line(s, c, yz - 1, gains, kernel, sums)
            apply_line(s, c, s.ny * s.half - 1, gains, kernel, sums)
            return carry

        lax.fori_loop(0, combos_x(s), functools.partial(along_x, True), 0, unroll=True)
        lax.fori_loop(combos_x(s), combos_x(s) + 2, functools.partial(along_x, False), 0, unroll=2)

        flow, weight = flow_of(s, sums, conduct_own[...], temp_own[...])
        flow_out[...] = flow
        occupied = own[3 * s.cells : 4 * s.cells, :] > 0.0
        top = jnp.max(jnp.where(occupied, weight, 0.0), axis=0, keepdims=True)
        top_out[...] = top
        faces.pack_x(flow_out, top, up, down)

    cells, padded = f32(s.cells, slots), f32(s.padded, slots)
    return pl.pallas_call(
        body,
        out_shape=(
            kernel_shape(s),
            cells,
            padded,
            padded,
            cells,
            cells,
            f32(1, slots),
            *faces.x_messages(),
        ),
        input_output_aliases={0: 0},
        scratch_shapes=[
            fields.halo_shape,
            pltpu.VMEM((s.columns * s.half, slots, 128), jnp.bfloat16),
            pltpu.VMEM((s.padded, 8, slots), jnp.float32),
            pltpu.VMEM((s.cells * 8, slots), jnp.float32),
            pltpu.VMEM((9, s.padded, slots), jnp.float32),
        ],
        compiler_params=pltpu.CompilerParams(vmem_limit_bytes=room),
        name="outer_and_first_flow",
    )


def part_kernel(s, room):
    slots = s.slots
    faces = Faces(s, 1)

    def body(kernel, volume, scaled, after, own, x0, x1, y0, y1, sums, temp, gains):
        faces.put_own(temp, own)
        faces.put_x(temp, x0, x1)
        faces.put_y(temp, y0, y1)
        none = jnp.zeros((1, slots), jnp.float32)
        for column in range(s.columns):
            for z in (0, s.pz - 1):
                temp[column * s.pz + z : column * s.pz + z + 1, :] = none
        source_rows(s, volume, scaled, temp, gains)
        sums[...] = jnp.zeros_like(sums)

        def along_x(c, carry):
            for yz in range(s.ny * s.half):
                apply_line(s, c, yz, gains, kernel, sums, inner_z)
            return carry

        lax.fori_loop(0, combos_x(s) + 2, along_x, 0, unroll=True)

    return pl.pallas_call(
        body,
        out_shape=f32(s.cells * 8, slots),
        scratch_shapes=[faces.halo_shape, pltpu.VMEM((s.padded, 8, slots), jnp.float32)],
        compiler_params=pltpu.CompilerParams(vmem_limit_bytes=room),
        name="part_flow",
    )


def next_kernel(s, room, last):
    slots = s.slots
    faces = Faces(s, 1)
    arrivals = len(faces.z_messages())

    def body(kernel, volume, scaled, conduct_own, part, *rest):
        if last:
            temp_own, flow1, *rest = rest
        own, top, x0, x1, y0, y1, *rest = rest
        z, rest = rest[:arrivals], rest[arrivals:]
        if last:
            out, temp, gains, sums, *rest = rest
        else:
            flow_out, top_out, up, down, temp, gains, sums = rest
        faces.lay_out(temp, own, x0, x1, y0, y1, z)
        most = faces.latest_top(top, z)
        source_rows(s, volume, scaled, temp, gains)

        sums[...] = part[...]

        def along_x(c, carry):
            for yz in range(s.ny * s.half):
                apply_line(s, c, yz, gains, kernel, sums, outer_z)
            return carry

        lax.fori_loop(0, combos_x(s) + 2, along_x, 0, unroll=True)
        flow, _ = flow_of(s, sums, conduct_own[...], own[...])
        if last and covered():
            rows, block, arrived = rest
            step = step_factor / jnp.max(most, axis=1, keepdims=True)
            rows[...] = polynomial(temp_own[...], step, flow1[...], own[...], flow)
            for x in range(s.nx):
                for y in range(s.ny):
                    start = (x * s.ny + y) * s.nz
                    block[x, y] = rows[start : start + s.nz, :]
            copy = pltpu.make_async_copy(block, out, arrived)
            copy.start()
            copy.wait()
        elif last:
            out[...] = flow
        else:
            flow_out[...] = flow
            top_out[...] = most
            faces.pack_x(flow_out, most, up, down)

    cells, shape = f32(s.cells, slots), (s.nx, s.ny, s.nz, slots)
    outs = (cells, f32(1, slots), *faces.x_messages())
    spaces = [pltpu.VMEM] * len(outs)
    scratch = [
        faces.halo_shape,
        pltpu.VMEM((s.padded, 8, slots), jnp.float32),
        pltpu.VMEM((s.cells * 8, slots), jnp.float32),
    ]
    if last and covered():
        outs, spaces = (f32(*shape),), [pl.ANY]
        scratch += [pltpu.VMEM((s.cells, slots), jnp.float32), pltpu.VMEM(shape, jnp.float32), pltpu.SemaphoreType.DMA]
    elif last:
        outs, spaces = (cells,), [pltpu.VMEM]
    return pl.pallas_call(
        body,
        out_shape=outs,
        out_specs=tuple(pl.BlockSpec(memory_space=space) for space in spaces),
        scratch_shapes=scratch,
        compiler_params=pltpu.CompilerParams(vmem_limit_bytes=room),
        name="last_flow" if last else "next_flow",
    )


def covered():
    return all(lax.axis_size(axis) <= 5 for axis in AXES)


def polynomial(start, step, flow1, flow2, flow3):
    return start + step * (flow1 + step * (0.5 * flow2 + step * (1.0 / 15.0) * flow3))


def local(relative_placements, mass_per_density, opening_heat_level, bin_fill_counts):
    nx, ny, nz, slots = opening_heat_level.shape
    s = Sizes(nx, ny, nz, slots)
    fields, faces = Faces(s, FIELDS), Faces(s, 1)
    arguments = (bin_fill_counts, relative_placements, mass_per_density, opening_heat_level)
    started = start_kernel(s)(*[pltpu.with_memory_space_constraint(a, pltpu.HBM) for a in arguments])
    made = []
    own_bytes = 4 * slots * rounded_up(FIELDS * s.cells)
    parts = (0, combos_x(s) // 7, 4 * combos_x(s) // 7, combos_x(s))

    def during(phase, after, *_):
        begin, end = parts[phase], parts[phase + 1]
        if phase == 0:
            *outs, done = inner_kernel(s, ROOM - own_bytes - 4096, begin, end)(started[0], after)
            made.extend(outs)
        else:
            made[0], done = inner_kernel(s, ROOM, begin, end)(*made, after)
        return done

    own, _, *messages = fields.exchange(*started, during)
    kernel, low, high, _ = made
    kernel, flow1, volume, scaled, conduct_own, temp_own, top, up, down = outer_kernel(s, ROOM - own_bytes)(
        kernel, low, high, own, *messages
    )
    sums = []

    def apply_part(phase, after, *messages):
        if phase == 2:
            sums.append(part_kernel(s, ROOM)(kernel, volume, scaled, after, *messages))

    arrived = faces.exchange(flow1, top, up, down, apply_part)
    flow2, top, up, down = next_kernel(s, ROOM, False)(kernel, volume, scaled, conduct_own, sums[0], *arrived)
    arrived = faces.exchange(flow2, top, up, down, apply_part)
    (final,) = next_kernel(s, ROOM, True)(
        kernel, volume, scaled, conduct_own, sums[1], temp_own, flow1, *arrived
    )
    if not covered():
        top, flow3 = lax.optimization_barrier((arrived[1], final))
        step = step_factor / lax.pmax(jnp.max(top), AXES)
        final = polynomial(temp_own, step, flow1, flow2, flow3).reshape(nx, ny, nz, slots)
    return final


def solution(mesh):
    in_specs = (
        P(None, "gx", "gy", "gz", None),
        P("gx", "gy", "gz", None),
        P("gx", "gy", "gz", None),
        P("gx", "gy", "gz"),
    )
    out_specs = P("gx", "gy", "gz", None)
    return jax.shard_map(local, mesh=mesh, in_specs=in_specs, out_specs=out_specs, check_vma=False)
```
